32 devices in a mesh: gx: 4 (over y, x), gy: 8 (over z, core).
Axes of the slice: x: 2, y: 2, z: 4, core: 2. Of those that a mesh axis runs over, the one named last changes fastest.
Arguments:
- point_coords: float32 [128, 3, 256], P(('gx', 'gy')), may hold values from -2 to 2
- charge: float32 [128, 256], P(('gx', 'gy')), may hold values from -0.12 to 0.12
- shell_index: int32 [128, 32, 256], P(('gx', 'gy')), may hold values from 0 to 63
- neighbours: int32 [128, 32], P(('gx', 'gy')), may hold values from 0 to 1023, as said below
- neighbour_count: int32 [128], P(('gx', 'gy')), may hold values from 24 to 32
- batch_load: int32 [32], P(('gx', 'gy')), may hold values from 3 to 4, as said below
- atom_coords: float32 [3, 1024], replicated, may hold values from -2 to 2
- owner_slot: int32 [1024], replicated, may hold values from 0 to 1023, as said below
Outputs:
- potential: float32 [128, 256], P(('gx', 'gy'))
- moments: float32 [1024, 3136], P(('gx', 'gy'))
The draws below stay inside these ranges and needn't reach their ends.
Inputs may be any that keep to these rules, and one draw needn't show every extreme that they name: `neighbours`: atom labels. On every device, at most 4 of its 128 neighbour slots, live or not, name atoms whose owner_slot lies in one block of 32 rows; on every device some block gets exactly 4. `owner_slot`: each row number once. `batch_load`: some device has all 4 slots live.
All inputs are finite; a program needn't handle non-finite values.
Results may differ from the reference program's by a relative error of at most 0.0003.
Values sent between devices are 32-bit elements; how exact they have to be, the bound alone decides.
No kernel may reach another device: no remote copies, remote signals or barrier semaphores. Data moves between devices by JAX's collectives and lax.ppermute only.
A program may use at most 64 MiB of HBM per device.

```python
import math
import jax
import jax.numpy as jnp
from jax import lax

LM = 49
SHELLS = 64
PTS = 256
NB = 32
BSLOT = 4
ATOM_DEV = 32
NBATCH = 128
ATOMS = 1024
CAP = 4
DEVICES = 32


def owner_table(key):
    return jax.random.permutation(jax.random.fold_in(key, 7), ATOMS).astype(jnp.int32)


def draw_owner_slot(key, part):
    return owner_table(key)


def draw_neighbours(key, part):
    table = owner_table(key)
    inverse = jnp.zeros((ATOMS,), jnp.int32).at[table].set(jnp.arange(ATOMS, dtype=jnp.int32))
    row_total = BSLOT * NB
    spaces = DEVICES * CAP

    def one_device(device_key):
        first_key, score_key, local_key, shuffle_key = jax.random.split(device_key, 4)
        chosen = jax.random.randint(first_key, (), 0, DEVICES)
        spot = jnp.arange(spaces, dtype=jnp.int32)
        target = spot // CAP
        noise = jax.random.randint(score_key, (spaces,), 1, 2 ** 20)
        scores = jnp.where(target == chosen, spot, noise * spaces + spot)
        ranked = jnp.argsort(scores)
        destination = target[ranked[:row_total]]
        destination = jax.random.permutation(shuffle_key, destination)
        local = jax.random.randint(local_key, (row_total,), 0, ATOM_DEV)
        return inverse[destination * ATOM_DEV + local].reshape(BSLOT, NB)
    keys = jax.random.split(jax.random.fold_in(key, 11), DEVICES)
    return jax.vmap(one_device)(keys).reshape(DEVICES * BSLOT, NB).astype(jnp.int32)


def draw_batch_load(key, part):
    loads = jax.random.randint(jax.random.fold_in(key, 3), (DEVICES,), 3 * BSLOT // 4, BSLOT + 1)
    busiest = jax.random.randint(jax.random.fold_in(key, 5), (), 0, DEVICES)
    return jnp.where(jnp.arange(DEVICES) == busiest, BSLOT, loads).astype(jnp.int32)


def place_ends(entries, own_key, low, high):
    place = [jax.random.randint(jax.random.fold_in(own_key, axis), (), 0, length) for axis, length in enumerate(entries.shape)]
    main_axis = entries.shape.index(max(entries.shape))
    next_to = place[:main_axis] + [(place[main_axis] + 1) % entries.shape[main_axis]] + place[main_axis + 1:]
    return entries.at[tuple(place)].set(low).at[tuple(next_to)].set(high)


def levels(own_key, extent, cuts, smallest, largest):
    def one(axis_at, shards_of):
        heights = jax.random.uniform(jax.random.fold_in(jax.random.fold_in(own_key, 6), axis_at), (shards_of,), jnp.float32, smallest / len(cuts), largest / len(cuts))
        return jnp.repeat(jnp.exp(heights), extent[axis_at] // shards_of).reshape((-1,) + (1,) * (len(extent) - axis_at - 1))

    gain = one(*cuts[0])
    for cut in cuts[1:]:
        gain = gain * one(*cut)
    return gain


def scatter_about(own_key, extent, spread, bound, cuts=(), kind=jnp.bfloat16):
    values = spread * jax.random.normal(own_key, extent, jnp.float32)
    if cuts:
        values = values * levels(own_key, extent, cuts, -0.22, 0.18)
    return jnp.clip(values, -bound, bound).astype(kind)


def setup_inputs(seed: int = 0) -> dict:
    splits = jax.random.split(jax.random.key(seed), 9)
    return {
        "point_coords": jnp.clip(jax.random.uniform(splits[0], (NBATCH, 3, PTS), jnp.float32, -2.0, 2.0) * levels(splits[0], (NBATCH, 3, PTS), ((0, 32),), -0.4, 0.0), -2.0, 2.0),
        "charge": scatter_about(splits[1], (NBATCH, PTS), 0.02, 0.12, ((0, 32),), jnp.float32),
        "shell_index": place_ends(jax.random.randint(splits[2], (NBATCH, NB, PTS), 0, SHELLS), jax.random.fold_in(splits[2], 1), 0, SHELLS - 1).astype(jnp.int32),
        "neighbours": draw_neighbours(jax.random.fold_in(splits[8], 71), 0),
        "neighbour_count": place_ends(jax.random.randint(splits[4], (NBATCH,), 3 * NB // 4, NB + 1), jax.random.fold_in(splits[4], 1), 3 * NB // 4, NB).astype(jnp.int32),
        "batch_load": draw_batch_load(jax.random.fold_in(splits[8], 71), 0),
        "atom_coords": jnp.clip(jax.random.uniform(splits[6], (3, ATOMS), jnp.float32, -2.0, 2.0), -2.0, 2.0),
        "owner_slot": draw_owner_slot(jax.random.fold_in(splits[8], 71), 0),
    }


SOFTEN = 0.01

def harmonics(along_x, along_y, along_z):
    cosines = [jnp.ones_like(along_x)]
    sines = [jnp.zeros_like(along_x)]
    for azimuth in range(1, 7):
        previous_cos = cosines[-1]
        previous_sin = sines[-1]
        cosines.append(previous_cos * along_x - previous_sin * along_y)
        sines.append(previous_cos * along_y + previous_sin * along_x)
    legendre = {}
    for azimuth in range(7):
        legendre[azimuth, azimuth] = jnp.ones_like(along_z) * float(math.prod(range(1, 2 * azimuth, 2)))
        if azimuth < 6:
            legendre[azimuth + 1, azimuth] = (2 * azimuth + 1) * along_z * legendre[azimuth, azimuth]
        for degree in range(azimuth + 2, 7):
            legendre[degree, azimuth] = ((2 * degree - 1) * along_z * legendre[degree - 1, azimuth] - (degree + azimuth - 1) * legendre[degree - 2, azimuth]) / (degree - azimuth)
    results = []
    for degree in range(7):
        for signed in range(-degree, degree + 1):
            azimuth = abs(signed)
            factor = math.sqrt((2 * degree + 1) / (4 * math.pi) * math.factorial(degree - azimuth) / math.factorial(degree + azimuth))
            if signed == 0:
                results.append(factor * legendre[degree, 0])
            elif signed > 0:
                results.append(math.sqrt(2.0) * factor * legendre[degree, azimuth] * cosines[azimuth])
            else:
                results.append(math.sqrt(2.0) * factor * legendre[degree, azimuth] * sines[azimuth])
    return jnp.stack(results)

def green_table():
    shell_rank = jnp.arange(SHELLS, dtype=jnp.float32)
    radius = 0.5 * jnp.exp(2.3 * shell_rank / SHELLS)
    nearer = jnp.minimum(radius[:, None], radius[None, :])
    farther = jnp.maximum(radius[:, None], radius[None, :])
    kernels = []
    for degree in range(7):
        kernel = 4.0 * math.pi / (2 * degree + 1) * nearer ** degree / farther ** (degree + 1)
        kernels.extend([kernel] * (2 * degree + 1))
    return jnp.stack(kernels)

def batch_geometry(coords, atom_place, count):
    offset = coords[:, None, :] - atom_place[:, :, None]
    squared = lax.optimization_barrier(jnp.sum(offset * offset, axis=0))
    scale = 1.0 / jnp.sqrt(squared + SOFTEN)
    harmonic = harmonics(offset[0] * scale, offset[1] * scale, offset[2] * scale)
    slot_live = jnp.arange(atom_place.shape[1], dtype=jnp.int32) < count
    closeness = jnp.where(slot_live[:, None], 1.0 / (1.0 + squared), 0.0)
    share = closeness / lax.optimization_barrier(jnp.sum(closeness, axis=0, keepdims=True))
    return (harmonic, share, slot_live)

def reference(point_coords, charge, shell_index, neighbours, neighbour_count, batch_load, atom_coords, owner_slot):
    total_batches = charge.shape[0]
    batch_rank = jnp.arange(total_batches, dtype=jnp.int32)
    live_batch = (batch_rank % BSLOT < batch_load[batch_rank // BSLOT]).astype(jnp.float32)
    slot_rank = jnp.arange(NB, dtype=jnp.int32)

    def forward(moments, inputs):
        coords, weights_here, shells_here, labels, count, live = inputs
        harmonic, share, slot_live = batch_geometry(coords, atom_coords[:, labels], count)
        weighted = harmonic * (share * weights_here[None, :] * live)[None]
        segment = (slot_rank[:, None] * SHELLS + shells_here).reshape(-1).astype(jnp.int32)
        data = jnp.transpose(weighted, (1, 2, 0)).reshape(-1, harmonic.shape[0])
        summed = jax.ops.segment_sum(data, segment, num_segments=NB * SHELLS)
        partial_value = jnp.transpose(summed.reshape(NB, SHELLS, -1), (0, 2, 1))
        moments = moments.at[owner_slot[labels]].add(partial_value)
        return (moments, None)
    start = jnp.zeros((ATOMS, LM, SHELLS), jnp.float32)
    moments, _ = lax.scan(forward, start, (point_coords, charge, shell_index, neighbours, neighbour_count, live_batch))
    tables = jnp.einsum('lst,alt->als', green_table(), moments, precision=lax.Precision.HIGHEST)

    def evaluate(inputs):
        coords, shells_here, labels, count, live = inputs
        harmonic, share, slot_live = batch_geometry(coords, atom_coords[:, labels], count)
        table_rows = tables[owner_slot[labels]]
        spots = jnp.broadcast_to(shells_here[:, None, :], (NB, table_rows.shape[1], shells_here.shape[1]))
        picked = jnp.take_along_axis(table_rows, spots, axis=2)
        total = lax.optimization_barrier(jnp.sum(picked * jnp.transpose(harmonic, (1, 0, 2)), axis=1))
        return lax.optimization_barrier(jnp.sum(jnp.where(slot_live[:, None], total, 0.0), axis=0)) * live
    potential = lax.map(evaluate, (point_coords, shell_index, neighbours, neighbour_count, live_batch))
    return (potential, moments.reshape(ATOMS, LM * SHELLS))
```

```python
import functools
import math

import jax
import jax.numpy as jnp
from jax import lax
from jax.experimental import pallas as pl
from jax.experimental.pallas import tpu as pltpu
from jax.sharding import PartitionSpec as P

SHELLS = 64
LMAX = 6
HARM = (LMAX + 1) ** 2
PAD = 56
SOFTEN = 0.01
LANES = 128
FIELDS = 8
VMEM = pl.BlockSpec(memory_space=pltpu.VMEM)
SMEM = pl.BlockSpec(memory_space=pltpu.SMEM)
F32 = jnp.float32
BF16 = jnp.bfloat16


def iota(shape, axis):
    return lax.broadcasted_iota(jnp.int32, shape, axis)


def three_parts(value):
    first = value.astype(BF16)
    rest = value - first.astype(F32)
    second = rest.astype(BF16)
    third = (rest - second.astype(F32)).astype(BF16)
    return first, second, third


def pack_kernel(
    devices, count_ref, load_ref, label_ref, coord_ref, charge_ref, shell_ref, atom_ref, slot_ref, out_ref, table_ref
):
    batches, slots = label_ref.shape
    rows = batches * slots
    atoms = atom_ref.shape[1]
    owned = atoms // devices
    per_peer = rows // devices
    halves = charge_ref.shape[1] // LANES
    stride = out_ref.shape[0] // devices

    table_ref[...] = jnp.zeros_like(table_ref)
    table_ref[0:3, :] = atom_ref[...]
    for tile in range(atoms // LANES):
        table_ref[3:4, tile * LANES : (tile + 1) * LANES] = slot_ref[tile : tile + 1, :].astype(F32)
    label = jnp.concatenate([label_ref[b : b + 1, :] for b in range(batches)], axis=1)
    label = jnp.broadcast_to(label, (8, rows))
    high = lax.shift_right_logical(label, 7)
    low = lax.bitwise_and(label, 127)
    found = jnp.zeros((8, rows), F32)
    for tile in range(atoms // LANES):
        piece = table_ref[:, tile * LANES : (tile + 1) * LANES]
        picked = jnp.take_along_axis(piece, low, axis=1, mode="promise_in_bounds")
        found = jnp.where(high == tile, picked, found)
    slot = found[3:4, :]
    owner = jnp.floor((slot + 0.5) * (1.0 / owned))
    local = slot - owner * owned

    lane = iota((1, rows), 1)
    batch_row = jnp.zeros((1, rows), F32)
    live_row = jnp.zeros((1, rows), F32)
    for b in range(batches):
        inside = (lane >= b * slots) & (lane < (b + 1) * slots)
        batch_row = jnp.where(inside, float(b), batch_row)
        alive = inside & (lane - b * slots < count_ref[b]) & (load_ref[0] > b)
        live_row = jnp.where(alive, 1.0, live_row)
    sub = iota((8, rows), 0)
    fields = found
    for place, value in ((3, local), (4, batch_row), (5, live_row), (6, owner)):
        fields = jnp.where(sub == place, jnp.broadcast_to(value, (8, rows)), fields)
    columns = jnp.concatenate([fields, jnp.zeros((LANES - 8, rows), F32)], axis=0).T

    owner_column = columns[:, 6:7]
    earlier = (owner_column == owner) & (iota((rows, rows), 0) < iota((rows, rows), 1))
    rank = jnp.sum(earlier.astype(F32), axis=0, keepdims=True)
    target = (rank * devices + owner).astype(jnp.int32)
    order = (iota((rows, rows), 0) == target).astype(F32).astype(BF16)

    shells = shell_ref[...].reshape(rows, halves * LANES).astype(F32).astype(BF16)
    moved = jnp.dot(order, shells, preferred_element_type=F32)
    meta = sum(jnp.dot(order, part, preferred_element_type=F32) for part in three_parts(columns))
    for group in range(devices // 8):
        base = group * 8 * stride
        total = jnp.zeros((8, LANES), F32)
        for c in range(per_peer):
            first = c * devices + group * 8
            for h in range(halves):
                out_ref[pl.ds(base + c * halves + h, 8, stride=stride), :] = moved[
                    first : first + 8, h * LANES : (h + 1) * LANES
                ]
            piece = meta[first : first + 8, :]
            total = total + (pltpu.roll(piece, FIELDS * c, 1) if c else piece)
        out_ref[pl.ds(base + stride - 1, 8, stride=stride), :] = total

    odd = lax.bitwise_and(iota((8, LANES), 0), 1) == 1
    slot_rank = iota((slots, 1), 0)
    for b in range(batches):
        squared = jnp.zeros((slots, halves * LANES), F32)
        for axis in range(3):
            place = columns[b * slots : (b + 1) * slots, axis : axis + 1]
            offset = coord_ref[axis, b : b + 1, :] - place
            squared = squared + offset * offset
        close = jnp.where(slot_rank < count_ref[b], 1.0 / (1.0 + squared), 0.0)
        live = jnp.where(load_ref[0] > b, 1.0, 0.0)
        weight = charge_ref[b : b + 1, :] * live / jnp.sum(close, axis=0, keepdims=True)
        for quantity in range(4):
            line = coord_ref[quantity, b : b + 1, :] if quantity < 3 else weight
            value = jnp.where(odd, line[:, LANES : 2 * LANES], line[:, 0:LANES])
            for group in range(devices // 8):
                at = group * 8 * stride + per_peer * halves + b * 4 + quantity
                out_ref[pl.ds(at, 8, stride=stride), :] = value


def harmonics(x, y, z):
    def factor(degree, azimuth):
        norm = math.sqrt(
            (2 * degree + 1) / (4 * math.pi) * math.factorial(degree - azimuth) / math.factorial(degree + azimuth)
        )
        return norm * (math.sqrt(2.0) if azimuth else 1.0)

    cosine, sine = None, None
    for azimuth in range(LMAX + 1):
        if azimuth == 1:
            cosine, sine = x, y
        elif azimuth > 1:
            cosine, sine = cosine * x - sine * y, cosine * y + sine * x
        older, newer = None, None
        for degree in range(azimuth, LMAX + 1):
            if degree == azimuth:
                value = float(math.prod(range(1, 2 * azimuth, 2))) * factor(degree, azimuth)
            elif degree == azimuth + 1:
                value = z * ((2 * azimuth + 1) * newer / factor(degree - 1, azimuth) * factor(degree, azimuth))
            else:
                up = (2 * degree - 1) / (degree - azimuth) * factor(degree, azimuth) / factor(degree - 1, azimuth)
                down = (degree + azimuth - 1) / (degree - azimuth) * factor(degree, azimuth) / factor(degree - 2, azimuth)
                value = (z * up) * newer - down * older
            older, newer = newer, value
            middle = degree * degree + degree
            if azimuth == 0:
                yield middle, value
            else:
                yield middle + azimuth, cosine * value
                yield middle - azimuth, sine * value


def two_parts(value):
    first = value.astype(BF16).astype(F32)
    return first, value - first


def owner_kernel(
    devices,
    per_peer,
    batches,
    parity_ref,
    own_ref,
    other_ref,
    moment_ref,
    reply_ref,
    y_own,
    y_other,
    w_own,
    w_other,
    hot_ref,
    sum_ref,
    table_ref,
    split_ref,
    part_own,
    part_other,
    meta_ref,
    meta_smem,
    sem,
):
    stride = own_ref.shape[0] // devices
    groups = devices // 8
    rows = devices * per_peer
    owned = moment_ref.shape[0]
    shell_rows = per_peer * 2
    parity = parity_ref[0]

    def gather_meta(group, carry):
        at = pl.multiple_of(group * 8, 8)
        line = own_ref[pl.ds(group * 8 * stride + stride - 1, 8, stride=stride), :]
        meta_ref[pl.ds(at, 8), :] = line.astype(jnp.int32)
        return carry

    lax.fori_loop(0, groups, gather_meta, 0)
    copy = pltpu.make_async_copy(meta_ref, meta_smem, sem)
    copy.start()

    sum_ref[...] = jnp.zeros_like(sum_ref)
    table_ref[...] = jnp.zeros_like(table_ref)

    def column(line, c, field):
        at = FIELDS * c + field
        return jnp.broadcast_to(line[:, at : at + 1], (8, LANES))

    def geometry(group, carry):
        base = group * 8 * stride
        line = own_ref[pl.ds(base + stride - 1, 8, stride=stride), :]
        for source, y_ref, w_ref in ((own_ref, y_own, w_own), (other_ref, y_other, w_other)):
            points = [
                [source[pl.ds(base + shell_rows + b * 4 + i, 8, stride=stride), :] for i in range(4)]
                for b in range(batches)
            ]
            for c in range(per_peer):
                batch = column(line, c, 4)
                chosen = list(points[0])
                for b in range(1, batches):
                    chosen = [jnp.where(batch == b, new, old) for new, old in zip(points[b], chosen)]
                offset = [chosen[i] - column(line, c, i) for i in range(3)]
                squared = offset[0] * offset[0] + offset[1] * offset[1] + offset[2] * offset[2]
                scale = lax.rsqrt(squared + SOFTEN)
                weight = jnp.where(column(line, c, 5) > 0.5, chosen[3] / (1.0 + squared), 0.0)
                w_ref[pl.ds(group * 8 * per_peer + c, 8, stride=per_peer), :] = weight
                start = (group * 8 * per_peer + c) * PAD
                for k, value in harmonics(*(part * scale for part in offset)):
                    y_ref[pl.ds(start + k, 8, stride=per_peer * PAD), :] = jnp.broadcast_to(value, (8, LANES))
                for k in range(HARM, PAD):
                    y_ref[pl.ds(start + k, 8, stride=per_peer * PAD), :] = jnp.zeros((8, LANES), F32)
        return carry

    lax.fori_loop(0, groups, geometry, 0)
    copy.wait()

    def forward(source, carry):
        for c in range(per_peer):
            row = source * per_peer + c
            first = pl.multiple_of(row * PAD, 8)
            weighted, hot = [], []
            for side, (y_ref, w_ref) in enumerate(((y_own, w_own), (y_other, w_other))):
                weighted.append(y_ref[pl.ds(first, PAD), :] * w_ref[pl.ds(row, 1), :])
                half = parity if side == 0 else 1 - parity
                shell = own_ref[pl.ds(source * stride + c * 2 + half, 1), :]
                hot.append((iota((SHELLS, LANES), 0).astype(F32) == shell).astype(F32))
            weighted = jnp.concatenate(weighted, axis=1).reshape(PAD // 8, 8, 2 * LANES)
            hot = jnp.concatenate(hot, axis=1).astype(BF16)
            hot_ref[pl.ds(pl.multiple_of(row * SHELLS, SHELLS), SHELLS), :] = hot
            both = jnp.concatenate(two_parts(weighted), axis=1).reshape(2 * PAD, 2 * LANES).astype(BF16)
            made = lax.dot_general(both, hot, (((1,), (1,)), ((), ())), preferred_element_type=F32)
            made = made.reshape(PAD // 8, 2, 8, SHELLS)
            made = (made[:, 0] + made[:, 1]).reshape(PAD, SHELLS)
            local = meta_smem[source, FIELDS * c + 3]
            at = pl.multiple_of(local * PAD, 8)
            sum_ref[pl.ds(at, PAD), 0:SHELLS] += made
        return carry

    lax.fori_loop(0, devices, forward, 0)

    left = iota((owned, LANES), 1) < SHELLS
    row_rank = iota((SHELLS, LANES), 0).astype(F32)
    lane_rank = iota((SHELLS, LANES), 1).astype(F32)
    ratio = jnp.exp(jnp.abs(row_rank - lane_rank) * (-2.3 / SHELLS))
    kernel = jnp.exp(jnp.maximum(row_rank, lane_rank) * (-2.3 / SHELLS)) * 2.0
    kernel = jnp.where(lane_rank < SHELLS, kernel, 0.0)
    before = None
    for degree in range(LMAX + 1):
        lines = []
        for k in range(degree * degree, (degree + 1) ** 2):
            line = sum_ref[pl.ds(k, owned, stride=PAD), :]
            lines.append(line)
            if k % 2 == 0:
                before = line
                if k == HARM - 1:
                    moment_ref[:, k * SHELLS : (k + 1) * SHELLS] = line[:, 0:SHELLS]
            else:
                moment_ref[:, (k - 1) * SHELLS : (k + 1) * SHELLS] = jnp.where(
                    left, before, pltpu.roll(line, SHELLS, 1)
                )
        green = kernel * (4.0 * math.pi / (2 * degree + 1))
        kernel = kernel * ratio
        g_first, g_second = two_parts(green)
        first, second = two_parts(jnp.concatenate(lines, axis=0))
        both = (first + pltpu.roll(second, SHELLS, 1)).astype(BF16)
        made = jnp.dot(both, jnp.concatenate([g_first, g_first], axis=0).astype(BF16), preferred_element_type=F32)
        made = made + jnp.dot(
            both, jnp.concatenate([g_second, g_second], axis=0).astype(BF16), preferred_element_type=F32
        )
        for place, k in enumerate(range(degree * degree, (degree + 1) ** 2)):
            table_ref[pl.ds(k, owned, stride=PAD), :] = made[place * owned : (place + 1) * owned, :]

    def split(atom, carry):
        first, second = two_parts(table_ref[pl.ds(pl.multiple_of(atom * PAD, 8), PAD), :])
        both = first + pltpu.roll(second, SHELLS, 1)
        both = jnp.concatenate([both, jnp.zeros((SHELLS - PAD, LANES), F32)], axis=0)
        split_ref[pl.ds(pl.multiple_of(atom * SHELLS, SHELLS), SHELLS), :] = both.astype(BF16)
        return carry

    lax.fori_loop(0, owned, split, 0)

    def evaluate(source, carry):
        for c in range(per_peer):
            row = source * per_peer + c
            local = meta_smem[source, FIELDS * c + 3]
            table = split_ref[pl.ds(pl.multiple_of(local * SHELLS, SHELLS), SHELLS), :]
            hot = hot_ref[pl.ds(pl.multiple_of(row * SHELLS, SHELLS), SHELLS), :]
            picked = jnp.dot(table, jnp.concatenate([hot, hot], axis=0), preferred_element_type=F32)
            first = pl.multiple_of(row * PAD, 8)
            at = pl.multiple_of(row * 8, 8)
            for side, (y_ref, part_ref) in enumerate(((y_own, part_own), (y_other, part_other))):
                product = picked[0:PAD, side * LANES : (side + 1) * LANES] * y_ref[pl.ds(first, PAD), :]
                part_ref[pl.ds(at, 8), :] = jnp.sum(product.reshape(PAD // 8, 8, LANES), axis=0)
        return carry

    lax.fori_loop(0, devices, evaluate, 0)

    def answer(group, carry):
        line = own_ref[pl.ds(group * 8 * stride + stride - 1, 8, stride=stride), :]
        for side, part_ref in enumerate((part_own, part_other)):
            half = parity if side == 0 else 1 - parity
            totals = [jnp.zeros((8, LANES), F32) for _ in range(batches)]
            for c in range(per_peer):
                start = (group * 8 * per_peer + c) * 8
                total = part_ref[pl.ds(start, 8, stride=per_peer * 8), :]
                for i in range(1, 8):
                    total = total + part_ref[pl.ds(start + i, 8, stride=per_peer * 8), :]
                total = jnp.where(column(line, c, 5) > 0.5, total, 0.0)
                batch = column(line, c, 4)
                totals = [old + jnp.where(batch == b, total, 0.0) for b, old in enumerate(totals)]
            for b in range(batches):
                at = group * 8 * (2 * batches) + half * batches + b
                reply_ref[pl.ds(at, 8, stride=2 * batches), :] = totals[b]
        return carry

    lax.fori_loop(0, groups, answer, 0)


def body(
    point_coords,
    charge,
    shell_index,
    neighbours,
    neighbour_count,
    batch_load,
    atom_coords,
    owner_slot,
):
    batches, slots = neighbours.shape
    points = charge.shape[1]
    atoms = owner_slot.shape[0]
    count_gy = lax.axis_size("gy")
    devices = lax.axis_size("gx") * count_gy
    owned = atoms // devices
    rows = batches * slots
    per_peer = rows // devices
    stride = per_peer * (points // LANES) + batches * 4 + 1

    outgoing = pl.pallas_call(
        functools.partial(pack_kernel, devices),
        out_shape=jax.ShapeDtypeStruct((devices * stride, LANES), F32),
        in_specs=[SMEM, SMEM] + [VMEM] * 6,
        out_specs=VMEM,
        scratch_shapes=[pltpu.VMEM((8, atoms), F32)],
        name="pack",
    )(
        neighbour_count,
        batch_load,
        neighbours,
        jnp.transpose(point_coords, (1, 0, 2)),
        charge,
        shell_index,
        atom_coords,
        owner_slot.reshape(atoms // LANES, LANES),
    )
    arrived = lax.all_to_all(
        outgoing.reshape(devices, stride, 1, LANES), ("gx", "gy"), split_axis=0, concat_axis=0, tiled=True
    ).reshape(devices * stride, LANES)
    swapped = lax.ppermute(arrived, "gy", [(i, i ^ 1) for i in range(count_gy)])
    parity = (lax.axis_index("gy") % 2).astype(jnp.int32).reshape(1)
    moments, reply = pl.pallas_call(
        functools.partial(owner_kernel, devices, per_peer, batches),
        out_shape=(
            jax.ShapeDtypeStruct((owned, HARM * SHELLS), F32),
            jax.ShapeDtypeStruct((devices * 2 * batches, LANES), F32),
        ),
        in_specs=[SMEM, VMEM, VMEM],
        out_specs=(VMEM, VMEM),
        scratch_shapes=[
            pltpu.VMEM((rows * PAD, LANES), F32),
            pltpu.VMEM((rows * PAD, LANES), F32),
            pltpu.VMEM((rows, LANES), F32),
            pltpu.VMEM((rows, LANES), F32),
            pltpu.VMEM((rows * SHELLS, 2 * LANES), BF16),
            pltpu.VMEM((owned * PAD, LANES), F32),
            pltpu.VMEM((owned * PAD, LANES), F32),
            pltpu.VMEM((owned * SHELLS, LANES), BF16),
            pltpu.VMEM((rows * 8, LANES), F32),
            pltpu.VMEM((rows * 8, LANES), F32),
            pltpu.VMEM((devices, LANES), jnp.int32),
            pltpu.SMEM((devices, LANES), jnp.int32),
            pltpu.SemaphoreType.DMA,
        ],
        compiler_params=pltpu.CompilerParams(vmem_limit_bytes=24 << 20),
        name="owner",
    )(parity, arrived, swapped)
    returned = lax.all_to_all(
        reply.reshape(devices, 2 * batches, LANES), ("gx", "gy"), split_axis=0, concat_axis=0, tiled=True
    )
    potential = jnp.sum(returned, axis=0).reshape(2, batches, LANES)
    return jnp.transpose(potential, (1, 0, 2)).reshape(batches, points), moments


def solution(mesh):
    return jax.shard_map(
        body,
        mesh=mesh,
        in_specs=(
            P(("gx", "gy"), None, None),
            P(("gx", "gy"), None),
            P(("gx", "gy"), None, None),
            P(("gx", "gy"), None),
            P(("gx", "gy")),
            P(("gx", "gy")),
            P(),
            P(),
        ),
        out_specs=(P(("gx", "gy"), None), P(("gx", "gy"), None)),
        check_vma=False,
    )
```

```python
import functools
import math

import jax
import jax.numpy as jnp
from jax import lax
from jax.experimental import pallas as pl
from jax.experimental.pallas import tpu as pltpu
from jax.sharding import PartitionSpec as P

SHELLS = 64
LMAX = 6
HARM = (LMAX + 1) ** 2
PAD = 56
SOFTEN = 0.01
LANES = 128
FIELDS = 8
BLOCK = 448
SPILL = 64
ROWS_AT_ONCE = 16
VMEM = pl.BlockSpec(memory_space=pltpu.VMEM)
SMEM = pl.BlockSpec(memory_space=pltpu.SMEM)
F32 = jnp.float32
BF16 = jnp.bfloat16


def iota(shape, axis):
    return lax.broadcasted_iota(jnp.int32, shape, axis)


def three_parts(value):
    first = value.astype(BF16)
    rest = value - first.astype(F32)
    second = rest.astype(BF16)
    third = (rest - second.astype(F32)).astype(BF16)
    return first, second, third


def pack_kernel(
    devices, count_ref, load_ref, label_ref, coord_ref, charge_ref, shell_ref, atom_ref, slot_ref, out_ref, table_ref
):
    batches, slots = label_ref.shape
    rows = batches * slots
    atoms = atom_ref.shape[1]
    owned = atoms // devices
    per_peer = rows // devices
    halves = charge_ref.shape[1] // LANES
    stride = out_ref.shape[0] // devices

    table_ref[...] = jnp.zeros_like(table_ref)
    table_ref[0:3, :] = atom_ref[...]
    for tile in range(atoms // LANES):
        table_ref[3:4, tile * LANES : (tile + 1) * LANES] = slot_ref[tile : tile + 1, :].astype(F32)
    label = jnp.concatenate([label_ref[b : b + 1, :] for b in range(batches)], axis=1)
    label = jnp.broadcast_to(label, (8, rows))
    high = lax.shift_right_logical(label, 7)
    low = lax.bitwise_and(label, 127)
    found = jnp.zeros((8, rows), F32)
    for tile in range(atoms // LANES):
        piece = table_ref[:, tile * LANES : (tile + 1) * LANES]
        picked = jnp.take_along_axis(piece, low, axis=1, mode="promise_in_bounds")
        found = jnp.where(high == tile, picked, found)
    slot = found[3:4, :]
    owner = jnp.floor((slot + 0.5) * (1.0 / owned))
    local = slot - owner * owned

    lane = iota((1, rows), 1)
    batch_row = jnp.zeros((1, rows), F32)
    live_row = jnp.zeros((1, rows), F32)
    for b in range(batches):
        inside = (lane >= b * slots) & (lane < (b + 1) * slots)
        batch_row = jnp.where(inside, float(b), batch_row)
        alive = inside & (lane - b * slots < count_ref[b]) & (load_ref[0] > b)
        live_row = jnp.where(alive, 1.0, live_row)
    sub = iota((8, rows), 0)
    fields = found
    for place, value in ((3, local), (4, batch_row), (5, live_row), (6, owner)):
        fields = jnp.where(sub == place, jnp.broadcast_to(value, (8, rows)), fields)
    columns = jnp.concatenate([fields, jnp.zeros((LANES - 8, rows), F32)], axis=0).T

    owner_column = columns[:, 6:7]
    earlier = (owner_column == owner) & (iota((rows, rows), 0) < iota((rows, rows), 1))
    rank = jnp.sum(earlier.astype(F32), axis=0, keepdims=True)
    target = (rank * devices + owner).astype(jnp.int32)
    order = (iota((rows, rows), 0) == target).astype(F32).astype(BF16)

    shells = shell_ref[...].reshape(rows, halves * LANES).astype(F32).astype(BF16)
    moved = jnp.dot(order, shells, preferred_element_type=F32)
    meta = sum(jnp.dot(order, part, preferred_element_type=F32) for part in three_parts(columns))
    for group in range(devices // 8):
        base = group * 8 * stride
        total = jnp.zeros((8, LANES), F32)
        for c in range(per_peer):
            first = c * devices + group * 8
            for h in range(halves):
                out_ref[pl.ds(base + c * halves + h, 8, stride=stride), :] = moved[
                    first : first + 8, h * LANES : (h + 1) * LANES
                ]
            piece = meta[first : first + 8, :]
            total = total + (pltpu.roll(piece, FIELDS * c, 1) if c else piece)
        out_ref[pl.ds(base + stride - 1, 8, stride=stride), :] = total

    odd = lax.bitwise_and(iota((8, LANES), 0), 1) == 1
    slot_rank = iota((slots, 1), 0)
    for b in range(batches):
        squared = jnp.zeros((slots, halves * LANES), F32)
        for axis in range(3):
            place = columns[b * slots : (b + 1) * slots, axis : axis + 1]
            offset = coord_ref[axis, b : b + 1, :] - place
            squared = squared + offset * offset
        close = jnp.where(slot_rank < count_ref[b], 1.0 / (1.0 + squared), 0.0)
        live = jnp.where(load_ref[0] > b, 1.0, 0.0)
        weight = charge_ref[b : b + 1, :] * live / jnp.sum(close, axis=0, keepdims=True)
        for quantity in range(4):
            line = coord_ref[quantity, b : b + 1, :] if quantity < 3 else weight
            value = jnp.where(odd, line[:, LANES : 2 * LANES], line[:, 0:LANES])
            for group in range(devices // 8):
                at = group * 8 * stride + per_peer * halves + b * 4 + quantity
                out_ref[pl.ds(at, 8, stride=stride), :] = value


def harmonics(x, y, z):
    def factor(degree, azimuth):
        norm = math.sqrt(
            (2 * degree + 1) / (4 * math.pi) * math.factorial(degree - azimuth) / math.factorial(degree + azimuth)
        )
        return norm * (math.sqrt(2.0) if azimuth else 1.0)

    cosine, sine = None, None
    for azimuth in range(LMAX + 1):
        if azimuth == 1:
            cosine, sine = x, y
        elif azimuth > 1:
            cosine, sine = cosine * x - sine * y, cosine * y + sine * x
        older, newer = None, None
        for degree in range(azimuth, LMAX + 1):
            if degree == azimuth:
                value = float(math.prod(range(1, 2 * azimuth, 2))) * factor(degree, azimuth)
            elif degree == azimuth + 1:
                value = z * ((2 * azimuth + 1) * newer / factor(degree - 1, azimuth) * factor(degree, azimuth))
            else:
                up = (2 * degree - 1) / (degree - azimuth) * factor(degree, azimuth) / factor(degree - 1, azimuth)
                down = (degree + azimuth - 1) / (degree - azimuth) * factor(degree, azimuth) / factor(degree - 2, azimuth)
                value = (z * up) * newer - down * older
            older, newer = newer, value
            middle = degree * degree + degree
            if azimuth == 0:
                yield middle, value
            else:
                yield middle + azimuth, cosine * value
                yield middle - azimuth, sine * value


def split_rows(value):
    main, tail = value[0 : PAD - 8], value[PAD - 8 : PAD]
    first = main.astype(BF16)
    second = (main - first.astype(F32)).astype(BF16)
    last = tail.astype(BF16).astype(F32)
    last = jnp.concatenate([last, tail - last], axis=0).astype(BF16)
    return jnp.concatenate([first, last, second], axis=0)


def join_rows(value):
    main = value[0 : PAD - 8] + value[PAD + 8 :]
    return jnp.concatenate([main, value[PAD - 8 : PAD] + value[PAD : PAD + 8]], axis=0)


def two_parts(value):
    first = value.astype(BF16).astype(F32)
    return first, value - first


def owner_kernel(
    devices,
    per_peer,
    batches,
    parity_ref,
    own_ref,
    other_ref,
    moment_hbm,
    reply_ref,
    y_own,
    y_other,
    w_own,
    w_other,
    sum_ref,
    table_ref,
    split_ref,
    part_own,
    part_other,
    moment_ref,
    meta_ref,
    meta_smem,
    sem,
    out_sem,
):
    stride = own_ref.shape[0] // devices
    groups = devices // 8
    owned = moment_ref.shape[0]
    pitch = owned + 1
    shell_rows = per_peer * 2
    parity = parity_ref[0]
    step = max(1, ROWS_AT_ONCE // per_peer)

    def gather_meta(group, carry):
        at = pl.multiple_of(group * 8, 8)
        line = own_ref[pl.ds(group * 8 * stride + stride - 1, 8, stride=stride), :]
        meta_ref[pl.ds(at, 8), :] = line.astype(jnp.int32)
        return carry

    lax.fori_loop(0, groups, gather_meta, 0)
    copy = pltpu.make_async_copy(meta_ref, meta_smem, sem)
    copy.start()

    sum_ref[...] = jnp.zeros_like(sum_ref)
    table_ref[...] = jnp.zeros_like(table_ref)
    for y_ref in (y_own, y_other):
        y_ref[pl.ds(devices * per_peer // 8 * BLOCK, SPILL), :] = jnp.zeros((SPILL, LANES), F32)

    def column(line, c, field):
        at = FIELDS * c + field
        return jnp.broadcast_to(line[:, at : at + 1], (8, LANES))

    def geometry(group, carry):
        base = group * 8 * stride
        line = own_ref[pl.ds(base + stride - 1, 8, stride=stride), :]
        for source, y_ref, w_ref in ((own_ref, y_own, w_own), (other_ref, y_other, w_other)):
            points = [
                [source[pl.ds(base + shell_rows + b * 4 + i, 8, stride=stride), :] for i in range(4)]
                for b in range(batches)
            ]
            for c in range(per_peer):
                batch = column(line, c, 4)
                chosen = list(points[0])
                for b in range(1, batches):
                    chosen = [jnp.where(batch == b, new, old) for new, old in zip(points[b], chosen)]
                offset = [chosen[i] - column(line, c, i) for i in range(3)]
                squared = offset[0] * offset[0] + offset[1] * offset[1] + offset[2] * offset[2]
                scale = lax.rsqrt(squared + SOFTEN)
                weight = jnp.where(column(line, c, 5) > 0.5, chosen[3] / (1.0 + squared), 0.0)
                w_ref[pl.ds(group * 8 * per_peer + c, 8, stride=per_peer), :] = weight
                start = pl.multiple_of((group * per_peer + c) * BLOCK, 8)
                for k, value in harmonics(*(part * scale for part in offset)):
                    y_ref[pl.ds(start + k * 9, 8), :] = jnp.broadcast_to(value, (8, LANES))
        return carry

    lax.fori_loop(0, groups, geometry, 0)
    copy.wait()

    def hot_shells(source, c):
        hot = []
        for side in range(2):
            half = parity if side == 0 else 1 - parity
            shell = own_ref[pl.ds(source * stride + c * 2 + half, 1), :]
            hot.append((iota((SHELLS, LANES), 0).astype(F32) == shell).astype(F32))
        return jnp.concatenate(hot, axis=1).astype(BF16)

    def harmonic_rows(source, c, y_ref):
        start = ((source // 8) * per_peer + c) * BLOCK + source % 8
        return y_ref[pl.ds(start, PAD, stride=9), :]

    def forward(turn, carry):
        for place in range(step * per_peer):
            source, c = turn * step + place // per_peer, place % per_peer
            row = source * per_peer + c
            weighted = [
                harmonic_rows(source, c, y_ref) * w_ref[pl.ds(row, 1), :]
                for y_ref, w_ref in ((y_own, w_own), (y_other, w_other))
            ]
            both = split_rows(jnp.concatenate(weighted, axis=1))
            made = lax.dot_general(
                both, hot_shells(source, c), (((1,), (1,)), ((), ())), preferred_element_type=F32
            )
            local = meta_smem[source, FIELDS * c + 3]
            sum_ref[pl.ds(local, PAD, stride=pitch), 0:SHELLS] += join_rows(made)
        return carry

    lax.fori_loop(0, devices // step, forward, 0)

    left = iota((owned, LANES), 1) < SHELLS
    row_rank = iota((SHELLS, LANES), 0).astype(F32)
    lane_rank = iota((SHELLS, LANES), 1).astype(F32)
    ratio = jnp.exp(jnp.abs(row_rank - lane_rank) * (-2.3 / SHELLS))
    kernel = jnp.exp(jnp.maximum(row_rank, lane_rank) * (-2.3 / SHELLS)) * 2.0
    kernel = jnp.where(lane_rank < SHELLS, kernel, 0.0)
    before = None
    for degree in range(LMAX + 1):
        lines = []
        for k in range(degree * degree, (degree + 1) ** 2):
            line = sum_ref[k * pitch : k * pitch + owned, :]
            lines.append(line)
            if k % 2 == 0:
                before = line
                if k == HARM - 1:
                    moment_ref[:, k * SHELLS : (k + 1) * SHELLS] = line[:, 0:SHELLS]
            else:
                moment_ref[:, (k - 1) * SHELLS : (k + 1) * SHELLS] = jnp.where(
                    left, before, pltpu.roll(line, SHELLS, 1)
                )
        green = kernel * (4.0 * math.pi / (2 * degree + 1))
        kernel = kernel * ratio
        g_first, g_second = two_parts(green)
        first, second = two_parts(jnp.concatenate(lines, axis=0))
        both = (first + pltpu.roll(second, SHELLS, 1)).astype(BF16)
        made = jnp.dot(both, jnp.concatenate([g_first, g_first], axis=0).astype(BF16), preferred_element_type=F32)
        made = made + jnp.dot(
            both, jnp.concatenate([g_second, g_second], axis=0).astype(BF16), preferred_element_type=F32
        )
        for place, k in enumerate(range(degree * degree, (degree + 1) ** 2)):
            table_ref[k * pitch : k * pitch + owned, :] = made[place * owned : (place + 1) * owned, :]
    result = pltpu.make_async_copy(moment_ref, moment_hbm, out_sem)
    result.start()

    def split(turn, carry):
        for place in range(8):
            atom = turn * 8 + place
            both = split_rows(table_ref[pl.ds(atom, PAD, stride=pitch), :])
            split_ref[pl.ds(pl.multiple_of(atom * 2 * PAD, 16), 2 * PAD), :] = both
        return carry

    lax.fori_loop(0, owned // 8, split, 0)

    def evaluate(turn, carry):
        for place in range(step * per_peer):
            source, c = turn * step + place // per_peer, place % per_peer
            local = meta_smem[source, FIELDS * c + 3]
            table = split_ref[pl.ds(pl.multiple_of(local * 2 * PAD, 16), 2 * PAD), 0:SHELLS]
            picked = join_rows(jnp.dot(table, hot_shells(source, c), preferred_element_type=F32))
            at = ((source // 8) * per_peer + c) * 72 + source % 8
            for side, (y_ref, part_ref) in enumerate(((y_own, part_own), (y_other, part_other))):
                product = picked[:, side * LANES : (side + 1) * LANES] * harmonic_rows(source, c, y_ref)
                part_ref[pl.ds(at, 8, stride=9), :] = jnp.sum(product.reshape(PAD // 8, 8, LANES), axis=0)
        return carry

    lax.fori_loop(0, devices // step, evaluate, 0)

    def answer(group, carry):
        line = own_ref[pl.ds(group * 8 * stride + stride - 1, 8, stride=stride), :]
        for side, part_ref in enumerate((part_own, part_other)):
            half = parity if side == 0 else 1 - parity
            totals = [jnp.zeros((8, LANES), F32) for _ in range(batches)]
            for c in range(per_peer):
                start = pl.multiple_of((group * per_peer + c) * 72, 8)
                total = part_ref[pl.ds(start, 8), :]
                for i in range(1, 8):
                    total = total + part_ref[pl.ds(start + 9 * i, 8), :]
                total = jnp.where(column(line, c, 5) > 0.5, total, 0.0)
                batch = column(line, c, 4)
                totals = [old + jnp.where(batch == b, total, 0.0) for b, old in enumerate(totals)]
            for b in range(batches):
                at = group * 8 * (2 * batches) + half * batches + b
                reply_ref[pl.ds(at, 8, stride=2 * batches), :] = totals[b]
        return carry

    lax.fori_loop(0, groups, answer, 0)
    result.wait()


def body(
    point_coords,
    charge,
    shell_index,
    neighbours,
    neighbour_count,
    batch_load,
    atom_coords,
    owner_slot,
):
    batches, slots = neighbours.shape
    points = charge.shape[1]
    atoms = owner_slot.shape[0]
    count_gy = lax.axis_size("gy")
    devices = lax.axis_size("gx") * count_gy
    owned = atoms // devices
    rows = batches * slots
    per_peer = rows // devices
    stride = per_peer * (points // LANES) + batches * 4 + 1

    outgoing = pl.pallas_call(
        functools.partial(pack_kernel, devices),
        out_shape=jax.ShapeDtypeStruct((devices * stride, LANES), F32),
        in_specs=[SMEM, SMEM] + [VMEM] * 6,
        out_specs=VMEM,
        scratch_shapes=[pltpu.VMEM((8, atoms), F32)],
        name="pack",
    )(
        neighbour_count,
        batch_load,
        neighbours,
        jnp.transpose(point_coords, (1, 0, 2)),
        charge,
        shell_index,
        atom_coords,
        owner_slot.reshape(atoms // LANES, LANES),
    )
    arrived = lax.all_to_all(
        outgoing.reshape(devices, stride, 1, LANES), ("gx", "gy"), split_axis=0, concat_axis=0, tiled=True
    ).reshape(devices * stride, LANES)
    swapped = lax.ppermute(arrived, "gy", [(i, i ^ 1) for i in range(count_gy)])
    parity = (lax.axis_index("gy") % 2).astype(jnp.int32).reshape(1)
    moments, reply = pl.pallas_call(
        functools.partial(owner_kernel, devices, per_peer, batches),
        out_shape=(
            jax.ShapeDtypeStruct((owned, HARM * SHELLS), F32),
            jax.ShapeDtypeStruct((devices * 2 * batches, LANES), F32),
        ),
        in_specs=[SMEM, VMEM, VMEM],
        out_specs=(pl.BlockSpec(memory_space=pltpu.HBM), VMEM),
        scratch_shapes=[
            pltpu.VMEM((rows // 8 * BLOCK + SPILL, LANES), F32),
            pltpu.VMEM((rows // 8 * BLOCK + SPILL, LANES), F32),
            pltpu.VMEM((rows, LANES), F32),
            pltpu.VMEM((rows, LANES), F32),
            pltpu.VMEM((PAD * (owned + 1), LANES), F32),
            pltpu.VMEM((PAD * (owned + 1), LANES), F32),
            pltpu.VMEM((owned * 2 * PAD, LANES), BF16),
            pltpu.VMEM((rows * 9, LANES), F32),
            pltpu.VMEM((rows * 9, LANES), F32),
            pltpu.VMEM((owned, HARM * SHELLS), F32),
            pltpu.VMEM((devices, LANES), jnp.int32),
            pltpu.SMEM((devices, LANES), jnp.int32),
            pltpu.SemaphoreType.DMA,
            pltpu.SemaphoreType.DMA,
        ],
        compiler_params=pltpu.CompilerParams(vmem_limit_bytes=24 << 20),
        name="owner",
    )(parity, arrived, swapped)
    returned = lax.all_to_all(
        reply.reshape(devices, 2 * batches, LANES), ("gx", "gy"), split_axis=0, concat_axis=0, tiled=True
    )
    potential = jnp.sum(returned, axis=0).reshape(2, batches, LANES)
    return jnp.transpose(potential, (1, 0, 2)).reshape(batches, points), moments


def solution(mesh):
    return jax.shard_map(
        body,
        mesh=mesh,
        in_specs=(
            P(("gx", "gy"), None, None),
            P(("gx", "gy"), None),
            P(("gx", "gy"), None, None),
            P(("gx", "gy"), None),
            P(("gx", "gy")),
            P(("gx", "gy")),
            P(),
            P(),
        ),
        out_specs=(P(("gx", "gy"), None), P(("gx", "gy"), None)),
        check_vma=False,
    )
```

```python
import functools
import math

import jax
import jax.numpy as jnp
from jax import lax
from jax.experimental import pallas as pl
from jax.experimental.pallas import tpu as pltpu
from jax.sharding import PartitionSpec as P

SHELLS = 64
LMAX = 6
HARM = (LMAX + 1) ** 2
PAD = 56
SOFTEN = 0.01
LANES = 128
FIELDS = 8
BLOCK = 448
SPILL = 64
ROWS_AT_ONCE = 128
VMEM = pl.BlockSpec(memory_space=pltpu.VMEM)
SMEM = pl.BlockSpec(memory_space=pltpu.SMEM)
HBM = pl.BlockSpec(memory_space=pltpu.HBM)
F32 = jnp.float32
BF16 = jnp.bfloat16


def iota(shape, axis):
    return lax.broadcasted_iota(jnp.int32, shape, axis)


def three_parts(value):
    first = value.astype(BF16)
    rest = value - first.astype(F32)
    second = rest.astype(BF16)
    third = (rest - second.astype(F32)).astype(BF16)
    return first, second, third


def pack_kernel(
    devices,
    load_ref,
    count_hbm,
    label_hbm,
    slot_hbm,
    atom_hbm,
    shell_hbm,
    coord_hbm,
    charge_hbm,
    out_ref,
    count_ref,
    label_ref,
    slot_ref,
    table_ref,
    shell_ref,
    coord_ref,
    charge_ref,
    sems,
):
    copies = [
        pltpu.make_async_copy(source, into, sems.at[place])
        for place, (source, into) in enumerate(
            (
                (label_hbm, label_ref),
                (slot_hbm, slot_ref),
                (atom_hbm, table_ref.at[0:3, :]),
                (shell_hbm, shell_ref),
                (coord_hbm, coord_ref),
                (charge_hbm, charge_ref),
                (count_hbm, count_ref),
            )
        )
    ]
    for copy in copies:
        copy.start()
    batches, slots = label_ref.shape
    rows = batches * slots
    atoms = table_ref.shape[1]
    owned = atoms // devices
    per_peer = rows // devices
    halves = charge_ref.shape[1] // LANES
    stride = out_ref.shape[0] // devices

    for copy in copies[0:3]:
        copy.wait()
    for tile in range(atoms // LANES):
        table_ref[3:4, tile * LANES : (tile + 1) * LANES] = slot_ref[tile : tile + 1, :].astype(F32)
    label = jnp.concatenate([label_ref[b : b + 1, :] for b in range(batches)], axis=1)
    label = jnp.broadcast_to(label, (8, rows))
    high = lax.shift_right_logical(label, 7)
    low = lax.bitwise_and(label, 127)
    kept = iota((8, rows), 0) < 4
    found = jnp.zeros((8, rows), F32)
    for tile in range(atoms // LANES):
        piece = table_ref[:, tile * LANES : (tile + 1) * LANES]
        picked = jnp.take_along_axis(piece, low, axis=1, mode="promise_in_bounds")
        found = jnp.where((high == tile) & kept, picked, found)
    slot = found[3:4, :]
    owner = jnp.floor((slot + 0.5) * (1.0 / owned))
    local = slot - owner * owned

    copies[6].wait()
    lane = iota((1, rows), 1)
    batch_row = jnp.zeros((1, rows), F32)
    live_row = jnp.zeros((1, rows), F32)
    for b in range(batches):
        inside = (lane >= b * slots) & (lane < (b + 1) * slots)
        batch_row = jnp.where(inside, float(b), batch_row)
        alive = inside & (lane - b * slots < count_ref[b]) & (load_ref[0] > b)
        live_row = jnp.where(alive, 1.0, live_row)
    sub = iota((8, rows), 0)
    fields = found
    for place, value in ((3, local), (4, batch_row), (5, live_row), (6, owner)):
        fields = jnp.where(sub == place, jnp.broadcast_to(value, (8, rows)), fields)
    columns = jnp.concatenate([fields, jnp.zeros((LANES - 8, rows), F32)], axis=0).T

    owner_column = columns[:, 6:7]
    earlier = (owner_column == owner) & (iota((rows, rows), 0) < iota((rows, rows), 1))
    rank = jnp.sum(earlier.astype(F32), axis=0, keepdims=True)
    target = (rank * devices + owner).astype(jnp.int32)
    order = (iota((rows, rows), 0) == target).astype(F32).astype(BF16)

    copies[3].wait()
    shells = shell_ref[...].reshape(rows, halves * LANES).astype(F32).astype(BF16)
    moved = jnp.dot(order, shells, preferred_element_type=F32)
    meta = sum(jnp.dot(order, part, preferred_element_type=F32) for part in three_parts(columns))
    for group in range(devices // 8):
        base = group * 8 * stride
        total = jnp.zeros((8, LANES), F32)
        for c in range(per_peer):
            first = c * devices + group * 8
            for h in range(halves):
                out_ref[pl.ds(base + c * halves + h, 8, stride=stride), :] = moved[
                    first : first + 8, h * LANES : (h + 1) * LANES
                ]
            piece = meta[first : first + 8, :]
            total = total + (pltpu.roll(piece, FIELDS * c, 1) if c else piece)
        out_ref[pl.ds(base + stride - 1, 8, stride=stride), :] = total

    copies[4].wait()
    copies[5].wait()
    odd = lax.bitwise_and(iota((8, LANES), 0), 1) == 1
    slot_rank = iota((slots, 1), 0)
    for b in range(batches):
        squared = jnp.zeros((slots, halves * LANES), F32)
        for axis in range(3):
            place = columns[b * slots : (b + 1) * slots, axis : axis + 1]
            offset = coord_ref[axis, b : b + 1, :] - place
            squared = squared + offset * offset
        close = jnp.where(slot_rank < count_ref[b], 1.0 / (1.0 + squared), 0.0)
        live = jnp.where(load_ref[0] > b, 1.0, 0.0)
        weight = charge_ref[b : b + 1, :] * live / jnp.sum(close, axis=0, keepdims=True)
        for quantity in range(4):
            line = coord_ref[quantity, b : b + 1, :] if quantity < 3 else weight
            value = jnp.where(odd, line[:, LANES : 2 * LANES], line[:, 0:LANES])
            for group in range(devices // 8):
                at = group * 8 * stride + per_peer * halves + b * 4 + quantity
                out_ref[pl.ds(at, 8, stride=stride), :] = value


def harmonics(x, y, z):
    def factor(degree, azimuth):
        norm = math.sqrt(
            (2 * degree + 1) / (4 * math.pi) * math.factorial(degree - azimuth) / math.factorial(degree + azimuth)
        )
        return norm * (math.sqrt(2.0) if azimuth else 1.0)

    cosine, sine = None, None
    for azimuth in range(LMAX + 1):
        if azimuth == 1:
            cosine, sine = x, y
        elif azimuth > 1:
            cosine, sine = cosine * x - sine * y, cosine * y + sine * x
        older, newer = None, None
        for degree in range(azimuth, LMAX + 1):
            if degree == azimuth:
                value = float(math.prod(range(1, 2 * azimuth, 2))) * factor(degree, azimuth)
            elif degree == azimuth + 1:
                value = z * ((2 * azimuth + 1) * newer / factor(degree - 1, azimuth) * factor(degree, azimuth))
            else:
                up = (2 * degree - 1) / (degree - azimuth) * factor(degree, azimuth) / factor(degree - 1, azimuth)
                down = (degree + azimuth - 1) / (degree - azimuth) * factor(degree, azimuth) / factor(degree - 2, azimuth)
                value = (z * up) * newer - down * older
            older, newer = newer, value
            middle = degree * degree + degree
            if azimuth == 0:
                yield middle, value
            else:
                yield middle + azimuth, cosine * value
                yield middle - azimuth, sine * value


def split_rows(value):
    main, tail = value[0 : PAD - 8], value[PAD - 8 : PAD]
    first = main.astype(BF16)
    second = (main - first.astype(F32)).astype(BF16)
    last = tail.astype(BF16).astype(F32)
    last = jnp.concatenate([last, tail - last], axis=0).astype(BF16)
    return jnp.concatenate([first, last, second], axis=0)


def join_rows(value):
    main = value[0 : PAD - 8] + value[PAD + 8 :]
    return jnp.concatenate([main, value[PAD - 8 : PAD] + value[PAD : PAD + 8]], axis=0)


def two_parts(value):
    first = value.astype(BF16).astype(F32)
    return first, value - first


def owner_kernel(
    devices,
    per_peer,
    batches,
    parity_ref,
    own_ref,
    other_ref,
    moment_hbm,
    reply_ref,
    y_own,
    y_other,
    w_own,
    w_other,
    sum_ref,
    table_ref,
    split_ref,
    part_own,
    part_other,
    moment_ref,
    meta_ref,
    meta_smem,
    sem,
    out_sem,
):
    stride = own_ref.shape[0] // devices
    groups = devices // 8
    owned = moment_ref.shape[0]
    pitch = owned + 1
    shell_rows = per_peer * 2
    parity = parity_ref[0]
    step = max(1, ROWS_AT_ONCE // per_peer)

    def gather_meta(group, carry):
        at = pl.multiple_of(group * 8, 8)
        line = own_ref[pl.ds(group * 8 * stride + stride - 1, 8, stride=stride), :]
        meta_ref[pl.ds(at, 8), :] = line.astype(jnp.int32)
        return carry

    lax.fori_loop(0, groups, gather_meta, 0)
    copy = pltpu.make_async_copy(meta_ref, meta_smem, sem)
    copy.start()

    sum_ref[...] = jnp.zeros_like(sum_ref)
    table_ref[HARM * pitch :, :] = jnp.zeros(((PAD - HARM) * pitch, LANES), F32)
    for y_ref in (y_own, y_other):
        y_ref[pl.ds(devices * per_peer // 8 * BLOCK, SPILL), :] = jnp.zeros((SPILL, LANES), F32)

    def column(line, c, field):
        at = FIELDS * c + field
        return jnp.broadcast_to(line[:, at : at + 1], (8, LANES))

    def geometry(group, carry):
        base = group * 8 * stride
        line = own_ref[pl.ds(base + stride - 1, 8, stride=stride), :]
        for source, y_ref, w_ref in ((own_ref, y_own, w_own), (other_ref, y_other, w_other)):
            points = [
                [source[pl.ds(base + shell_rows + b * 4 + i, 8, stride=stride), :] for i in range(4)]
                for b in range(batches)
            ]
            for c in range(per_peer):
                batch = column(line, c, 4)
                chosen = list(points[0])
                for b in range(1, batches):
                    chosen = [jnp.where(batch == b, new, old) for new, old in zip(points[b], chosen)]
                offset = [chosen[i] - column(line, c, i) for i in range(3)]
                squared = offset[0] * offset[0] + offset[1] * offset[1] + offset[2] * offset[2]
                scale = lax.rsqrt(squared + SOFTEN)
                weight = jnp.where(column(line, c, 5) > 0.5, chosen[3] / (1.0 + squared), 0.0)
                w_ref[pl.ds(group * 8 * per_peer + c, 8, stride=per_peer), :] = weight
                start = pl.multiple_of((group * per_peer + c) * BLOCK, 8)
                for k, value in harmonics(*(part * scale for part in offset)):
                    y_ref[pl.ds(start + k * 9, 8), :] = jnp.broadcast_to(value, (8, LANES))
        return carry

    lax.fori_loop(0, groups, geometry, 0)
    copy.wait()

    def hot_shells(source, c):
        hot = []
        for side in range(2):
            half = parity if side == 0 else 1 - parity
            shell = own_ref[pl.ds(source * stride + c * 2 + half, 1), :]
            hot.append((iota((SHELLS, LANES), 0).astype(F32) == shell).astype(F32))
        return jnp.concatenate(hot, axis=1).astype(BF16)

    def harmonic_rows(source, c, y_ref):
        start = ((source // 8) * per_peer + c) * BLOCK + source % 8
        return y_ref[pl.ds(start, PAD, stride=9), :]

    def forward(turn, carry):
        for place in range(step * per_peer):
            source, c = turn * step + place // per_peer, place % per_peer
            row = source * per_peer + c
            weighted = [
                harmonic_rows(source, c, y_ref) * w_ref[pl.ds(row, 1), :]
                for y_ref, w_ref in ((y_own, w_own), (y_other, w_other))
            ]
            both = split_rows(jnp.concatenate(weighted, axis=1))
            made = lax.dot_general(
                both, hot_shells(source, c), (((1,), (1,)), ((), ())), preferred_element_type=F32
            )
            local = meta_smem[source, FIELDS * c + 3]
            sum_ref[pl.ds(local, PAD, stride=pitch), 0:SHELLS] += join_rows(made)
        return carry

    lax.fori_loop(0, devices // step, forward, 0)

    left = iota((owned, LANES), 1) < SHELLS
    row_rank = iota((SHELLS, LANES), 0).astype(F32)
    lane_rank = iota((SHELLS, LANES), 1).astype(F32)
    lane_rank = jnp.where(lane_rank < SHELLS, lane_rank, lane_rank - SHELLS)
    ratio = jnp.exp(jnp.abs(row_rank - lane_rank) * (-2.3 / SHELLS))
    kernel = jnp.exp(jnp.maximum(row_rank, lane_rank) * (-2.3 / SHELLS)) * 2.0
    before = None
    for degree in range(LMAX + 1):
        lines = []
        for k in range(degree * degree, (degree + 1) ** 2):
            line = sum_ref[k * pitch : k * pitch + owned, :]
            lines.append(line)
            if k % 2 == 0:
                before = line
                if k == HARM - 1:
                    moment_ref[:, k * SHELLS : (k + 1) * SHELLS] = line[:, 0:SHELLS]
            else:
                moment_ref[:, (k - 1) * SHELLS : (k + 1) * SHELLS] = jnp.where(
                    left, before, pltpu.roll(line, SHELLS, 1)
                )
        green = kernel * (4.0 * math.pi / (2 * degree + 1))
        kernel = kernel * ratio
        g_first, g_second = two_parts(green)
        first, second = two_parts(jnp.concatenate(lines, axis=0))
        both = (first + pltpu.roll(second, SHELLS, 1)).astype(BF16)
        made = jnp.dot(both, jnp.concatenate([g_first, g_first], axis=0).astype(BF16), preferred_element_type=F32)
        made = made + jnp.dot(
            both, jnp.concatenate([g_second, g_second], axis=0).astype(BF16), preferred_element_type=F32
        )
        for place, k in enumerate(range(degree * degree, (degree + 1) ** 2)):
            table_ref[k * pitch : k * pitch + owned, :] = made[place * owned : (place + 1) * owned, :]
    result = pltpu.make_async_copy(moment_ref, moment_hbm, out_sem)
    result.start()

    def split(turn, carry):
        for place in range(8):
            atom = turn * 8 + place
            first, second = two_parts(table_ref[pl.ds(atom, PAD, stride=pitch), :])
            both = jnp.where(iota((PAD, LANES), 1) < SHELLS, first, second)
            both = jnp.concatenate([both, jnp.zeros((SHELLS - PAD, LANES), F32)], axis=0)
            split_ref[pl.ds(pl.multiple_of(atom * SHELLS, SHELLS), SHELLS), :] = both.astype(BF16)
        return carry

    lax.fori_loop(0, owned // 8, split, 0)

    def evaluate(turn, carry):
        for place in range(step * per_peer):
            source, c = turn * step + place // per_peer, place % per_peer
            local = meta_smem[source, FIELDS * c + 3]
            table = split_ref[pl.ds(pl.multiple_of(local * SHELLS, SHELLS), SHELLS), :]
            hot = hot_shells(source, c)
            picked = jnp.dot(table, jnp.concatenate([hot, hot], axis=0), preferred_element_type=F32)
            at = ((source // 8) * per_peer + c) * 72 + source % 8
            for side, (y_ref, part_ref) in enumerate(((y_own, part_own), (y_other, part_other))):
                product = picked[0:PAD, side * LANES : (side + 1) * LANES] * harmonic_rows(source, c, y_ref)
                part_ref[pl.ds(at, 8, stride=9), :] = jnp.sum(product.reshape(PAD // 8, 8, LANES), axis=0)
        return carry

    lax.fori_loop(0, devices // step, evaluate, 0)

    def answer(group, carry):
        line = own_ref[pl.ds(group * 8 * stride + stride - 1, 8, stride=stride), :]
        for side, part_ref in enumerate((part_own, part_other)):
            half = parity if side == 0 else 1 - parity
            totals = [jnp.zeros((8, LANES), F32) for _ in range(batches)]
            for c in range(per_peer):
                start = pl.multiple_of((group * per_peer + c) * 72, 8)
                total = part_ref[pl.ds(start, 8), :]
                for i in range(1, 8):
                    total = total + part_ref[pl.ds(start + 9 * i, 8), :]
                total = jnp.where(column(line, c, 5) > 0.5, total, 0.0)
                batch = column(line, c, 4)
                totals = [old + jnp.where(batch == b, total, 0.0) for b, old in enumerate(totals)]
            for b in range(batches):
                at = group * 8 * (2 * batches) + half * batches + b
                reply_ref[pl.ds(at, 8, stride=2 * batches), :] = totals[b]
        return carry

    lax.fori_loop(0, groups, answer, 0)
    result.wait()


def body(
    point_coords,
    charge,
    shell_index,
    neighbours,
    neighbour_count,
    batch_load,
    atom_coords,
    owner_slot,
):
    batches, slots = neighbours.shape
    points = charge.shape[1]
    atoms = owner_slot.shape[0]
    count_gy = lax.axis_size("gy")
    devices = lax.axis_size("gx") * count_gy
    owned = atoms // devices
    rows = batches * slots
    per_peer = rows // devices
    stride = per_peer * (points // LANES) + batches * 4 + 1

    outgoing = pl.pallas_call(
        functools.partial(pack_kernel, devices),
        out_shape=jax.ShapeDtypeStruct((devices * stride, LANES), F32),
        in_specs=[SMEM] + [HBM] * 7,
        out_specs=VMEM,
        scratch_shapes=[
            pltpu.SMEM((batches,), jnp.int32),
            pltpu.VMEM((batches, slots), jnp.int32),
            pltpu.VMEM((atoms // LANES, LANES), jnp.int32),
            pltpu.VMEM((8, atoms), F32),
            pltpu.VMEM((batches, slots, points), jnp.int32),
            pltpu.VMEM((3, batches, points), F32),
            pltpu.VMEM((batches, points), F32),
            pltpu.SemaphoreType.DMA((7,)),
        ],
        compiler_params=pltpu.CompilerParams(vmem_limit_bytes=16 << 20),
        name="pack",
    )(
        batch_load,
        *(
            pltpu.with_memory_space_constraint(value, pltpu.HBM)
            for value in (
                neighbour_count,
                neighbours,
                owner_slot.reshape(atoms // LANES, LANES),
                atom_coords,
                shell_index,
                jnp.transpose(point_coords, (1, 0, 2)),
                charge,
            )
        ),
    )
    arrived = lax.all_to_all(
        outgoing.reshape(devices, stride, 1, LANES), ("gx", "gy"), split_axis=0, concat_axis=0, tiled=True
    ).reshape(devices * stride, LANES)
    swapped = lax.ppermute(arrived, "gy", [(i, i ^ 1) for i in range(count_gy)])
    parity = (lax.axis_index("gy") % 2).astype(jnp.int32).reshape(1)
    moments, reply = pl.pallas_call(
        functools.partial(owner_kernel, devices, per_peer, batches),
        out_shape=(
            jax.ShapeDtypeStruct((owned, HARM * SHELLS), F32),
            jax.ShapeDtypeStruct((devices * 2 * batches, LANES), F32),
        ),
        in_specs=[SMEM, VMEM, VMEM],
        out_specs=(HBM, VMEM),
        scratch_shapes=[
            pltpu.VMEM((rows // 8 * BLOCK + SPILL, LANES), F32),
            pltpu.VMEM((rows // 8 * BLOCK + SPILL, LANES), F32),
            pltpu.VMEM((rows, LANES), F32),
            pltpu.VMEM((rows, LANES), F32),
            pltpu.VMEM((PAD * (owned + 1), LANES), F32),
            pltpu.VMEM((PAD * (owned + 1), LANES), F32),
            pltpu.VMEM((owned * SHELLS, LANES), BF16),
            pltpu.VMEM((rows * 9, LANES), F32),
            pltpu.VMEM((rows * 9, LANES), F32),
            pltpu.VMEM((owned, HARM * SHELLS), F32),
            pltpu.VMEM((devices, LANES), jnp.int32),
            pltpu.SMEM((devices, LANES), jnp.int32),
            pltpu.SemaphoreType.DMA,
            pltpu.SemaphoreType.DMA,
        ],
        compiler_params=pltpu.CompilerParams(vmem_limit_bytes=24 << 20),
        name="owner",
    )(parity, arrived, swapped)
    returned = lax.all_to_all(
        reply.reshape(devices, 2 * batches, LANES), ("gx", "gy"), split_axis=0, concat_axis=0, tiled=True
    )
    potential = jnp.sum(returned, axis=0).reshape(2, batches, LANES)
    return jnp.transpose(potential, (1, 0, 2)).reshape(batches, points), moments


def solution(mesh):
    return jax.shard_map(
        body,
        mesh=mesh,
        in_specs=(
            P(("gx", "gy"), None, None),
            P(("gx", "gy"), None),
            P(("gx", "gy"), None, None),
            P(("gx", "gy"), None),
            P(("gx", "gy")),
            P(("gx", "gy")),
            P(),
            P(),
        ),
        out_specs=(P(("gx", "gy"), None), P(("gx", "gy"), None)),
        check_vma=False,
    )
```

```python
import functools
import math

import jax
import jax.numpy as jnp
from jax import lax
from jax.experimental import pallas as pl
from jax.experimental.pallas import tpu as pltpu
from jax.sharding import PartitionSpec as P

SHELLS = 64
LMAX = 6
HARM = (LMAX + 1) ** 2
PAD = 56
SOFTEN = 0.01
LANES = 128
FIELDS = 8
BLOCK = 448
SPILL = 64
ROWS_AT_ONCE = 128
VMEM = pl.BlockSpec(memory_space=pltpu.VMEM)
SMEM = pl.BlockSpec(memory_space=pltpu.SMEM)
HBM = pl.BlockSpec(memory_space=pltpu.HBM)
F32 = jnp.float32
BF16 = jnp.bfloat16


def iota(shape, axis):
    return lax.broadcasted_iota(jnp.int32, shape, axis)


def three_parts(value):
    first = value.astype(BF16)
    rest = value - first.astype(F32)
    second = rest.astype(BF16)
    third = (rest - second.astype(F32)).astype(BF16)
    return first, second, third


def pack_kernel(
    devices,
    load_ref,
    count_hbm,
    label_hbm,
    slot_hbm,
    atom_hbm,
    shell_hbm,
    coord_hbm,
    charge_hbm,
    out_ref,
    count_ref,
    label_ref,
    slot_ref,
    table_ref,
    shell_ref,
    coord_ref,
    charge_ref,
    sems,
):
    copies = [
        pltpu.make_async_copy(source, into, sems.at[place])
        for place, (source, into) in enumerate(
            (
                (label_hbm, label_ref),
                (slot_hbm, slot_ref),
                (atom_hbm, table_ref.at[0:3, :]),
                (shell_hbm, shell_ref),
                (coord_hbm, coord_ref),
                (charge_hbm, charge_ref),
                (count_hbm, count_ref),
            )
        )
    ]
    for copy in copies:
        copy.start()
    batches, slots = label_ref.shape
    rows = batches * slots
    atoms = table_ref.shape[1]
    owned = atoms // devices
    per_peer = rows // devices
    halves = charge_ref.shape[1] // LANES
    stride = out_ref.shape[0] // devices

    for copy in copies[0:3]:
        copy.wait()
    for tile in range(atoms // LANES):
        table_ref[3:4, tile * LANES : (tile + 1) * LANES] = slot_ref[tile : tile + 1, :].astype(F32)
    label = jnp.concatenate([label_ref[b : b + 1, :] for b in range(batches)], axis=1)
    label = jnp.broadcast_to(label, (8, rows))
    high = lax.shift_right_logical(label, 7)
    low = lax.bitwise_and(label, 127)
    kept = iota((8, rows), 0) < 4
    found = jnp.zeros((8, rows), F32)
    for tile in range(atoms // LANES):
        piece = table_ref[:, tile * LANES : (tile + 1) * LANES]
        picked = jnp.take_along_axis(piece, low, axis=1, mode="promise_in_bounds")
        found = jnp.where((high == tile) & kept, picked, found)
    slot = found[3:4, :]
    owner = jnp.floor((slot + 0.5) * (1.0 / owned))
    local = slot - owner * owned

    for copy in copies[3:]:
        copy.wait()
    lane = iota((1, rows), 1)
    batch_row = jnp.zeros((1, rows), F32)
    live_row = jnp.zeros((1, rows), F32)
    for b in range(batches):
        inside = (lane >= b * slots) & (lane < (b + 1) * slots)
        batch_row = jnp.where(inside, float(b), batch_row)
        alive = inside & (lane - b * slots < count_ref[b]) & (load_ref[0] > b)
        live_row = jnp.where(alive, 1.0, live_row)
    sub = iota((8, rows), 0)
    fields = found
    for place, value in ((3, local), (4, batch_row), (5, live_row), (6, owner)):
        fields = jnp.where(sub == place, jnp.broadcast_to(value, (8, rows)), fields)
    columns = jnp.concatenate([fields, jnp.zeros((LANES - 8, rows), F32)], axis=0).T

    owner_column = columns[:, 6:7]
    earlier = (owner_column == owner) & (iota((rows, rows), 0) < iota((rows, rows), 1))
    rank = jnp.sum(earlier.astype(F32), axis=0, keepdims=True)
    target = (rank * devices + owner).astype(jnp.int32)
    order = (iota((rows, rows), 0) == target).astype(F32).astype(BF16)

    shells = shell_ref[...].reshape(rows, halves * LANES).astype(F32).astype(BF16)
    moved = jnp.dot(order, shells, preferred_element_type=F32)
    meta = sum(jnp.dot(order, part, preferred_element_type=F32) for part in three_parts(columns))
    for group in range(devices // 8):
        base = group * 8 * stride
        total = jnp.zeros((8, LANES), F32)
        for c in range(per_peer):
            first = c * devices + group * 8
            for h in range(halves):
                out_ref[pl.ds(base + c * halves + h, 8, stride=stride), :] = moved[
                    first : first + 8, h * LANES : (h + 1) * LANES
                ]
            piece = meta[first : first + 8, :]
            total = total + (pltpu.roll(piece, FIELDS * c, 1) if c else piece)
        out_ref[pl.ds(base + stride - 1, 8, stride=stride), :] = total

    odd = lax.bitwise_and(iota((8, LANES), 0), 1) == 1
    slot_rank = iota((slots, 1), 0)
    for b in range(batches):
        squared = jnp.zeros((slots, halves * LANES), F32)
        for axis in range(3):
            place = columns[b * slots : (b + 1) * slots, axis : axis + 1]
            offset = coord_ref[axis, b : b + 1, :] - place
            squared = squared + offset * offset
        close = jnp.where(slot_rank < count_ref[b], 1.0 / (1.0 + squared), 0.0)
        live = jnp.where(load_ref[0] > b, 1.0, 0.0)
        weight = charge_ref[b : b + 1, :] * live / jnp.sum(close, axis=0, keepdims=True)
        for quantity in range(4):
            line = coord_ref[quantity, b : b + 1, :] if quantity < 3 else weight
            value = jnp.where(odd, line[:, LANES : 2 * LANES], line[:, 0:LANES])
            for group in range(devices // 8):
                at = group * 8 * stride + per_peer * halves + b * 4 + quantity
                out_ref[pl.ds(at, 8, stride=stride), :] = value


def harmonics(x, y, z):
    def factor(degree, azimuth):
        norm = math.sqrt(
            (2 * degree + 1) / (4 * math.pi) * math.factorial(degree - azimuth) / math.factorial(degree + azimuth)
        )
        return norm * (math.sqrt(2.0) if azimuth else 1.0)

    cosine, sine = None, None
    for azimuth in range(LMAX + 1):
        if azimuth == 1:
            cosine, sine = x, y
        elif azimuth > 1:
            cosine, sine = cosine * x - sine * y, cosine * y + sine * x
        older, newer = None, None
        for degree in range(azimuth, LMAX + 1):
            if degree == azimuth:
                value = float(math.prod(range(1, 2 * azimuth, 2))) * factor(degree, azimuth)
            elif degree == azimuth + 1:
                value = z * ((2 * azimuth + 1) * newer / factor(degree - 1, azimuth) * factor(degree, azimuth))
            else:
                up = (2 * degree - 1) / (degree - azimuth) * factor(degree, azimuth) / factor(degree - 1, azimuth)
                down = (degree + azimuth - 1) / (degree - azimuth) * factor(degree, azimuth) / factor(degree - 2, azimuth)
                value = (z * up) * newer - down * older
            older, newer = newer, value
            middle = degree * degree + degree
            if azimuth == 0:
                yield middle, value
            else:
                yield middle + azimuth, cosine * value
                yield middle - azimuth, sine * value


def split_rows(value):
    main, tail = value[0 : PAD - 8], value[PAD - 8 : PAD]
    first = main.astype(BF16)
    second = (main - first.astype(F32)).astype(BF16)
    last = tail.astype(BF16).astype(F32)
    last = jnp.concatenate([last, tail - last], axis=0).astype(BF16)
    return jnp.concatenate([first, last, second], axis=0)


def join_rows(value):
    main = value[0 : PAD - 8] + value[PAD + 8 :]
    return jnp.concatenate([main, value[PAD - 8 : PAD] + value[PAD : PAD + 8]], axis=0)


def two_parts(value):
    first = value.astype(BF16).astype(F32)
    return first, value - first


def column(line, c, field):
    at = FIELDS * c + field
    return jnp.broadcast_to(line[:, at : at + 1], (8, LANES))


def geometry(devices, per_peer, batches, own_ref, source, y_ref, w_ref):
    stride = own_ref.shape[0] // devices
    shell_rows = per_peer * 2
    y_ref[pl.ds(devices * per_peer // 8 * BLOCK, SPILL), :] = jnp.zeros((SPILL, LANES), F32)

    def one(group, carry):
        base = group * 8 * stride
        line = own_ref[pl.ds(base + stride - 1, 8, stride=stride), :]
        points = [
            [source[pl.ds(base + shell_rows + b * 4 + i, 8, stride=stride), :] for i in range(4)]
            for b in range(batches)
        ]
        for c in range(per_peer):
            batch = column(line, c, 4)
            chosen = list(points[0])
            for b in range(1, batches):
                chosen = [jnp.where(batch == b, new, old) for new, old in zip(points[b], chosen)]
            offset = [chosen[i] - column(line, c, i) for i in range(3)]
            squared = offset[0] * offset[0] + offset[1] * offset[1] + offset[2] * offset[2]
            scale = lax.rsqrt(squared + SOFTEN)
            weight = jnp.where(column(line, c, 5) > 0.5, chosen[3] / (1.0 + squared), 0.0)
            w_ref[pl.ds(group * 8 * per_peer + c, 8, stride=per_peer), :] = weight
            start = pl.multiple_of((group * per_peer + c) * BLOCK, 8)
            for k, value in harmonics(*(part * scale for part in offset)):
                y_ref[pl.ds(start + k * 9, 8), :] = jnp.broadcast_to(value, (8, LANES))
        return carry

    lax.fori_loop(0, devices // 8, one, 0)


def own_kernel(devices, per_peer, batches, own_ref, y_ref, w_ref):
    geometry(devices, per_peer, batches, own_ref, own_ref, y_ref, w_ref)


def owner_kernel(
    devices,
    per_peer,
    batches,
    parity_ref,
    own_ref,
    other_ref,
    y_own,
    w_own,
    moment_hbm,
    reply_ref,
    y_other,
    w_other,
    sum_ref,
    table_ref,
    split_ref,
    part_own,
    part_other,
    moment_ref,
    meta_ref,
    meta_smem,
    sem,
    out_sem,
):
    stride = own_ref.shape[0] // devices
    groups = devices // 8
    owned = moment_ref.shape[0]
    pitch = owned + 1
    parity = parity_ref[0]
    step = max(1, ROWS_AT_ONCE // per_peer)

    def gather_meta(group, carry):
        at = pl.multiple_of(group * 8, 8)
        line = own_ref[pl.ds(group * 8 * stride + stride - 1, 8, stride=stride), :]
        meta_ref[pl.ds(at, 8), :] = line.astype(jnp.int32)
        return carry

    lax.fori_loop(0, groups, gather_meta, 0)
    copy = pltpu.make_async_copy(meta_ref, meta_smem, sem)
    copy.start()

    sum_ref[...] = jnp.zeros_like(sum_ref)
    table_ref[HARM * pitch :, :] = jnp.zeros(((PAD - HARM) * pitch, LANES), F32)

    geometry(devices, per_peer, batches, own_ref, other_ref, y_other, w_other)
    copy.wait()

    def hot_shells(source, c):
        hot = []
        for side in range(2):
            half = parity if side == 0 else 1 - parity
            shell = own_ref[pl.ds(source * stride + c * 2 + half, 1), :]
            hot.append((iota((SHELLS, LANES), 0).astype(F32) == shell).astype(F32))
        return jnp.concatenate(hot, axis=1).astype(BF16)

    def harmonic_rows(source, c, y_ref):
        start = ((source // 8) * per_peer + c) * BLOCK + source % 8
        return y_ref[pl.ds(start, PAD, stride=9), :]

    def forward(turn, carry):
        for place in range(step * per_peer):
            source, c = turn * step + place // per_peer, place % per_peer
            row = source * per_peer + c
            weighted = [
                harmonic_rows(source, c, y_ref) * w_ref[pl.ds(row, 1), :]
                for y_ref, w_ref in ((y_own, w_own), (y_other, w_other))
            ]
            both = split_rows(jnp.concatenate(weighted, axis=1))
            made = lax.dot_general(
                both, hot_shells(source, c), (((1,), (1,)), ((), ())), preferred_element_type=F32
            )
            local = meta_smem[source, FIELDS * c + 3]
            sum_ref[pl.ds(local, PAD, stride=pitch), 0:SHELLS] += join_rows(made)
        return carry

    lax.fori_loop(0, devices // step, forward, 0)

    left = iota((owned, LANES), 1) < SHELLS
    row_rank = iota((SHELLS, LANES), 0).astype(F32)
    lane_rank = iota((SHELLS, LANES), 1).astype(F32)
    lane_rank = jnp.where(lane_rank < SHELLS, lane_rank, lane_rank - SHELLS)
    ratio = jnp.exp(jnp.abs(row_rank - lane_rank) * (-2.3 / SHELLS))
    kernel = jnp.exp(jnp.maximum(row_rank, lane_rank) * (-2.3 / SHELLS)) * 2.0
    before = None
    for degree in range(LMAX + 1):
        lines = []
        for k in range(degree * degree, (degree + 1) ** 2):
            line = sum_ref[k * pitch : k * pitch + owned, :]
            line = line + pltpu.roll(line, SHELLS, 1)
            lines.append(line)
            if k == HARM - 1:
                moment_ref[:, k * SHELLS : (k + 1) * SHELLS] = line[:, 0:SHELLS]
            elif k % 2 == 0:
                before = line
            else:
                moment_ref[:, (k - 1) * SHELLS : (k + 1) * SHELLS] = jnp.where(left, before, line)
        green = kernel * (4.0 * math.pi / (2 * degree + 1))
        kernel = kernel * ratio
        green = jnp.concatenate(two_parts(green), axis=1).astype(BF16)
        first, second = two_parts(jnp.concatenate(lines, axis=0))
        both = jnp.where(iota(first.shape, 1) < SHELLS, first, second).astype(BF16)
        made = jnp.dot(both, jnp.concatenate([green, green], axis=0), preferred_element_type=F32)
        made = made[:, 0:LANES] + made[:, LANES : 2 * LANES]
        for place, k in enumerate(range(degree * degree, (degree + 1) ** 2)):
            table_ref[k * pitch : k * pitch + owned, :] = made[place * owned : (place + 1) * owned, :]
    result = pltpu.make_async_copy(moment_ref, moment_hbm, out_sem)
    result.start()

    def split(turn, carry):
        for place in range(8):
            atom = turn * 8 + place
            first, second = two_parts(table_ref[pl.ds(atom, PAD, stride=pitch), :])
            both = jnp.where(iota((PAD, LANES), 1) < SHELLS, first, second)
            both = jnp.concatenate([both, jnp.zeros((SHELLS - PAD, LANES), F32)], axis=0)
            split_ref[pl.ds(pl.multiple_of(atom * SHELLS, SHELLS), SHELLS), :] = both.astype(BF16)
        return carry

    lax.fori_loop(0, owned // 8, split, 0)

    def evaluate(turn, carry):
        for place in range(step * per_peer):
            source, c = turn * step + place // per_peer, place % per_peer
            local = meta_smem[source, FIELDS * c + 3]
            table = split_ref[pl.ds(pl.multiple_of(local * SHELLS, SHELLS), SHELLS), :]
            hot = hot_shells(source, c)
            picked = jnp.dot(table, jnp.concatenate([hot, hot], axis=0), preferred_element_type=F32)
            at = ((source // 8) * per_peer + c) * 72 + source % 8
            for side, (y_ref, part_ref) in enumerate(((y_own, part_own), (y_other, part_other))):
                product = picked[0:PAD, side * LANES : (side + 1) * LANES] * harmonic_rows(source, c, y_ref)
                part_ref[pl.ds(at, 8, stride=9), :] = jnp.sum(product.reshape(PAD // 8, 8, LANES), axis=0)
        return carry

    lax.fori_loop(0, devices // step, evaluate, 0)

    def answer(group, carry):
        line = own_ref[pl.ds(group * 8 * stride + stride - 1, 8, stride=stride), :]
        for side, part_ref in enumerate((part_own, part_other)):
            half = parity if side == 0 else 1 - parity
            totals = [jnp.zeros((8, LANES), F32) for _ in range(batches)]
            for c in range(per_peer):
                start = pl.multiple_of((group * per_peer + c) * 72, 8)
                total = part_ref[pl.ds(start, 8), :]
                for i in range(1, 8):
                    total = total + part_ref[pl.ds(start + 9 * i, 8), :]
                total = jnp.where(column(line, c, 5) > 0.5, total, 0.0)
                batch = column(line, c, 4)
                totals = [old + jnp.where(batch == b, total, 0.0) for b, old in enumerate(totals)]
            for b in range(batches):
                at = group * 8 * (2 * batches) + half * batches + b
                reply_ref[pl.ds(at, 8, stride=2 * batches), :] = totals[b]
        return carry

    lax.fori_loop(0, groups, answer, 0)
    result.wait()


def body(
    point_coords,
    charge,
    shell_index,
    neighbours,
    neighbour_count,
    batch_load,
    atom_coords,
    owner_slot,
):
    batches, slots = neighbours.shape
    points = charge.shape[1]
    atoms = owner_slot.shape[0]
    count_gy = lax.axis_size("gy")
    devices = lax.axis_size("gx") * count_gy
    owned = atoms // devices
    rows = batches * slots
    per_peer = rows // devices
    stride = per_peer * (points // LANES) + batches * 4 + 1

    outgoing = pl.pallas_call(
        functools.partial(pack_kernel, devices),
        out_shape=jax.ShapeDtypeStruct((devices * stride, LANES), F32),
        in_specs=[SMEM] + [HBM] * 7,
        out_specs=VMEM,
        scratch_shapes=[
            pltpu.SMEM((batches,), jnp.int32),
            pltpu.VMEM((batches, slots), jnp.int32),
            pltpu.VMEM((atoms // LANES, LANES), jnp.int32),
            pltpu.VMEM((8, atoms), F32),
            pltpu.VMEM((batches, slots, points), jnp.int32),
            pltpu.VMEM((3, batches, points), F32),
            pltpu.VMEM((batches, points), F32),
            pltpu.SemaphoreType.DMA((7,)),
        ],
        compiler_params=pltpu.CompilerParams(vmem_limit_bytes=16 << 20),
        name="pack",
    )(
        batch_load,
        *(
            pltpu.with_memory_space_constraint(value, pltpu.HBM)
            for value in (
                neighbour_count,
                neighbours,
                owner_slot.reshape(atoms // LANES, LANES),
                atom_coords,
                shell_index,
                jnp.transpose(point_coords, (1, 0, 2)),
                charge,
            )
        ),
    )
    arrived = lax.all_to_all(
        outgoing.reshape(devices, stride, 1, LANES), ("gx", "gy"), split_axis=0, concat_axis=0, tiled=True
    ).reshape(devices * stride, LANES)
    swapped = lax.ppermute(arrived, "gy", [(i, i ^ 1) for i in range(count_gy)])
    parity = (lax.axis_index("gy") % 2).astype(jnp.int32).reshape(1)
    held = rows // 8 * BLOCK + SPILL
    y_own, w_own = pl.pallas_call(
        functools.partial(own_kernel, devices, per_peer, batches),
        out_shape=(jax.ShapeDtypeStruct((held, LANES), F32), jax.ShapeDtypeStruct((rows, LANES), F32)),
        in_specs=[VMEM],
        out_specs=(VMEM, VMEM),
        compiler_params=pltpu.CompilerParams(vmem_limit_bytes=24 << 20),
        cost_estimate=pl.CostEstimate(flops=2_000_000_000, bytes_accessed=1000, transcendentals=0),
        name="own",
    )(arrived)
    moments, reply = pl.pallas_call(
        functools.partial(owner_kernel, devices, per_peer, batches),
        out_shape=(
            jax.ShapeDtypeStruct((owned, HARM * SHELLS), F32),
            jax.ShapeDtypeStruct((devices * 2 * batches, LANES), F32),
        ),
        in_specs=[SMEM] + [VMEM] * 4,
        out_specs=(HBM, VMEM),
        scratch_shapes=[
            pltpu.VMEM((held, LANES), F32),
            pltpu.VMEM((rows, LANES), F32),
            pltpu.VMEM((PAD * (owned + 1), LANES), F32),
            pltpu.VMEM((PAD * (owned + 1), LANES), F32),
            pltpu.VMEM((owned * SHELLS, LANES), BF16),
            pltpu.VMEM((rows * 9, LANES), F32),
            pltpu.VMEM((rows * 9, LANES), F32),
            pltpu.VMEM((owned, HARM * SHELLS), F32),
            pltpu.VMEM((devices, LANES), jnp.int32),
            pltpu.SMEM((devices, LANES), jnp.int32),
            pltpu.SemaphoreType.DMA,
            pltpu.SemaphoreType.DMA,
        ],
        compiler_params=pltpu.CompilerParams(vmem_limit_bytes=24 << 20),
        name="owner",
    )(parity, arrived, swapped, y_own, w_own)
    returned = lax.all_to_all(
        reply.reshape(devices, 2 * batches, LANES), ("gx", "gy"), split_axis=0, concat_axis=0, tiled=True
    )
    potential = jnp.sum(returned, axis=0).reshape(2, batches, LANES)
    return jnp.transpose(potential, (1, 0, 2)).reshape(batches, points), moments


def solution(mesh):
    return jax.shard_map(
        body,
        mesh=mesh,
        in_specs=(
            P(("gx", "gy"), None, None),
            P(("gx", "gy"), None),
            P(("gx", "gy"), None, None),
            P(("gx", "gy"), None),
            P(("gx", "gy")),
            P(("gx", "gy")),
            P(),
            P(),
        ),
        out_specs=(P(("gx", "gy"), None), P(("gx", "gy"), None)),
        check_vma=False,
    )
```

```python
import functools
import math

import jax
import jax.numpy as jnp
from jax import lax
from jax.experimental import pallas as pl
from jax.experimental.pallas import tpu as pltpu
from jax.sharding import PartitionSpec as P

SHELLS = 64
LMAX = 6
HARM = (LMAX + 1) ** 2
PAD = 56
SOFTEN = 0.01
LANES = 128
FIELDS = 8
BLOCK = 448
SPILL = 64
ROWS_AT_ONCE = 128
VMEM = pl.BlockSpec(memory_space=pltpu.VMEM)
SMEM = pl.BlockSpec(memory_space=pltpu.SMEM)
HBM = pl.BlockSpec(memory_space=pltpu.HBM)
F32 = jnp.float32
BF16 = jnp.bfloat16


def iota(shape, axis):
    return lax.broadcasted_iota(jnp.int32, shape, axis)


def three_parts(value):
    first = value.astype(BF16)
    rest = value - first.astype(F32)
    second = rest.astype(BF16)
    third = (rest - second.astype(F32)).astype(BF16)
    return first, second, third


def pack_kernel(
    devices,
    load_ref,
    count_hbm,
    label_hbm,
    slot_hbm,
    atom_hbm,
    shell_hbm,
    coord_hbm,
    charge_hbm,
    out_ref,
    count_ref,
    label_ref,
    slot_ref,
    table_ref,
    shell_ref,
    coord_ref,
    charge_ref,
    sems,
):
    copies = [
        pltpu.make_async_copy(source, into, sems.at[place])
        for place, (source, into) in enumerate(
            (
                (label_hbm, label_ref),
                (slot_hbm, slot_ref),
                (atom_hbm, table_ref.at[0:3, :]),
                (shell_hbm, shell_ref),
                (coord_hbm, coord_ref),
                (charge_hbm, charge_ref),
                (count_hbm, count_ref),
            )
        )
    ]
    for copy in copies:
        copy.start()
    batches, slots = label_ref.shape
    rows = batches * slots
    atoms = table_ref.shape[1]
    owned = atoms // devices
    per_peer = rows // devices
    halves = charge_ref.shape[1] // LANES
    stride = out_ref.shape[0] // devices

    for copy in copies[0:3]:
        copy.wait()
    for tile in range(atoms // LANES):
        table_ref[3:4, tile * LANES : (tile + 1) * LANES] = slot_ref[tile : tile + 1, :].astype(F32)
    label = jnp.concatenate([label_ref[b : b + 1, :] for b in range(batches)], axis=1)
    label = jnp.broadcast_to(label, (8, rows))
    high = lax.shift_right_logical(label, 7)
    low = lax.bitwise_and(label, 127)
    kept = iota((8, rows), 0) < 4
    found = jnp.zeros((8, rows), F32)
    for tile in range(atoms // LANES):
        piece = table_ref[:, tile * LANES : (tile + 1) * LANES]
        picked = jnp.take_along_axis(piece, low, axis=1, mode="promise_in_bounds")
        found = jnp.where((high == tile) & kept, picked, found)
    slot = found[3:4, :]
    owner = jnp.floor((slot + 0.5) * (1.0 / owned))
    local = slot - owner * owned

    for copy in copies[3:]:
        copy.wait()
    lane = iota((1, rows), 1)
    batch_row = jnp.zeros((1, rows), F32)
    live_row = jnp.zeros((1, rows), F32)
    for b in range(batches):
        inside = (lane >= b * slots) & (lane < (b + 1) * slots)
        batch_row = jnp.where(inside, float(b), batch_row)
        alive = inside & (lane - b * slots < count_ref[b]) & (load_ref[0] > b)
        live_row = jnp.where(alive, 1.0, live_row)
    sub = iota((8, rows), 0)
    fields = found
    for place, value in ((3, local), (4, batch_row), (5, live_row), (6, owner)):
        fields = jnp.where(sub == place, jnp.broadcast_to(value, (8, rows)), fields)
    columns = jnp.concatenate([fields, jnp.zeros((LANES - 8, rows), F32)], axis=0).T

    owner_column = columns[:, 6:7]
    earlier = (owner_column == owner) & (iota((rows, rows), 0) < iota((rows, rows), 1))
    rank = jnp.sum(earlier.astype(F32), axis=0, keepdims=True)
    target = (rank * devices + owner).astype(jnp.int32)
    order = (iota((rows, rows), 0) == target).astype(F32).astype(BF16)

    shells = shell_ref[...].reshape(rows, halves * LANES).astype(F32).astype(BF16)
    moved = jnp.dot(order, shells, preferred_element_type=F32)
    meta = sum(jnp.dot(order, part, preferred_element_type=F32) for part in three_parts(columns))
    for group in range(devices // 8):
        base = group * 8 * stride
        total = jnp.zeros((8, LANES), F32)
        for c in range(per_peer):
            first = c * devices + group * 8
            for h in range(halves):
                out_ref[pl.ds(base + c * halves + h, 8, stride=stride), :] = moved[
                    first : first + 8, h * LANES : (h + 1) * LANES
                ]
            piece = meta[first : first + 8, :]
            total = total + (pltpu.roll(piece, FIELDS * c, 1) if c else piece)
        out_ref[pl.ds(base + stride - 1, 8, stride=stride), :] = total

    odd = lax.bitwise_and(iota((8, LANES), 0), 1) == 1
    slot_rank = iota((slots, 1), 0)
    for b in range(batches):
        squared = jnp.zeros((slots, halves * LANES), F32)
        for axis in range(3):
            place = columns[b * slots : (b + 1) * slots, axis : axis + 1]
            offset = coord_ref[axis, b : b + 1, :] - place
            squared = squared + offset * offset
        close = jnp.where(slot_rank < count_ref[b], 1.0 / (1.0 + squared), 0.0)
        live = jnp.where(load_ref[0] > b, 1.0, 0.0)
        weight = charge_ref[b : b + 1, :] * live / jnp.sum(close, axis=0, keepdims=True)
        for quantity in range(4):
            line = coord_ref[quantity, b : b + 1, :] if quantity < 3 else weight
            value = jnp.where(odd, line[:, LANES : 2 * LANES], line[:, 0:LANES])
            for group in range(devices // 8):
                at = group * 8 * stride + per_peer * halves + b * 4 + quantity
                out_ref[pl.ds(at, 8, stride=stride), :] = value


def harmonics(x, y, z):
    def factor(degree, azimuth):
        norm = math.sqrt(
            (2 * degree + 1) / (4 * math.pi) * math.factorial(degree - azimuth) / math.factorial(degree + azimuth)
        )
        return norm * (math.sqrt(2.0) if azimuth else 1.0)

    cosine, sine = None, None
    for azimuth in range(LMAX + 1):
        if azimuth == 1:
            cosine, sine = x, y
        elif azimuth > 1:
            cosine, sine = cosine * x - sine * y, cosine * y + sine * x
        older, newer = None, None
        for degree in range(azimuth, LMAX + 1):
            if degree == azimuth:
                value = float(math.prod(range(1, 2 * azimuth, 2))) * factor(degree, azimuth)
            elif degree == azimuth + 1:
                value = z * ((2 * azimuth + 1) * newer / factor(degree - 1, azimuth) * factor(degree, azimuth))
            else:
                up = (2 * degree - 1) / (degree - azimuth) * factor(degree, azimuth) / factor(degree - 1, azimuth)
                down = (degree + azimuth - 1) / (degree - azimuth) * factor(degree, azimuth) / factor(degree - 2, azimuth)
                value = (z * up) * newer - down * older
            older, newer = newer, value
            middle = degree * degree + degree
            if azimuth == 0:
                yield middle, value
            else:
                yield middle + azimuth, cosine * value
                yield middle - azimuth, sine * value


def split_rows(value):
    main, tail = value[0 : PAD - 8], value[PAD - 8 : PAD]
    first = main.astype(BF16)
    second = (main - first.astype(F32)).astype(BF16)
    last = tail.astype(BF16).astype(F32)
    last = jnp.concatenate([last, tail - last], axis=0).astype(BF16)
    return jnp.concatenate([first, last, second], axis=0)


def join_rows(value):
    main = value[0 : PAD - 8] + value[PAD + 8 :]
    return jnp.concatenate([main, value[PAD - 8 : PAD] + value[PAD : PAD + 8]], axis=0)


def two_parts(value):
    first = value.astype(BF16).astype(F32)
    return first, value - first


def column(line, c, field):
    at = FIELDS * c + field
    return jnp.broadcast_to(line[:, at : at + 1], (8, LANES))


def geometry(devices, per_peer, batches, own_ref, source, y_ref, w_ref):
    stride = own_ref.shape[0] // devices
    shell_rows = per_peer * 2
    y_ref[pl.ds(devices * per_peer // 8 * BLOCK, SPILL), :] = jnp.zeros((SPILL, LANES), F32)

    def one(group, carry):
        base = group * 8 * stride
        line = own_ref[pl.ds(base + stride - 1, 8, stride=stride), :]
        points = [
            [source[pl.ds(base + shell_rows + b * 4 + i, 8, stride=stride), :] for i in range(4)]
            for b in range(batches)
        ]
        for c in range(per_peer):
            batch = column(line, c, 4)
            chosen = list(points[0])
            for b in range(1, batches):
                chosen = [jnp.where(batch == b, new, old) for new, old in zip(points[b], chosen)]
            offset = [chosen[i] - column(line, c, i) for i in range(3)]
            squared = offset[0] * offset[0] + offset[1] * offset[1] + offset[2] * offset[2]
            scale = lax.rsqrt(squared + SOFTEN)
            weight = jnp.where(column(line, c, 5) > 0.5, chosen[3] / (1.0 + squared), 0.0)
            w_ref[pl.ds(group * 8 * per_peer + c, 8, stride=per_peer), :] = weight
            start = pl.multiple_of((group * per_peer + c) * BLOCK, 8)
            for k, value in harmonics(*(part * scale for part in offset)):
                y_ref[pl.ds(start + k * 9, 8), :] = jnp.broadcast_to(value, (8, LANES))
        return carry

    lax.fori_loop(0, devices // 8, one, 0)


def own_kernel(devices, per_peer, batches, own_ref, y_ref, w_ref):
    geometry(devices, per_peer, batches, own_ref, own_ref, y_ref, w_ref)


def owner_kernel(
    devices,
    per_peer,
    batches,
    parity_ref,
    own_ref,
    other_ref,
    y_own,
    w_own,
    moment_hbm,
    reply_ref,
    y_other,
    w_other,
    sum_ref,
    table_ref,
    split_ref,
    part_own,
    part_other,
    moment_ref,
    meta_ref,
    meta_smem,
    sem,
    out_sem,
):
    stride = own_ref.shape[0] // devices
    groups = devices // 8
    owned = moment_ref.shape[0]
    pitch = owned + 1
    parity = parity_ref[0]
    step = max(1, ROWS_AT_ONCE // per_peer)

    def gather_meta(group, carry):
        at = pl.multiple_of(group * 8, 8)
        line = own_ref[pl.ds(group * 8 * stride + stride - 1, 8, stride=stride), :]
        meta_ref[pl.ds(at, 8), :] = line.astype(jnp.int32)
        return carry

    lax.fori_loop(0, groups, gather_meta, 0)
    copy = pltpu.make_async_copy(meta_ref, meta_smem, sem)
    copy.start()

    sum_ref[...] = jnp.zeros_like(sum_ref)
    table_ref[HARM * pitch :, :] = jnp.zeros(((PAD - HARM) * pitch, LANES), F32)

    geometry(devices, per_peer, batches, own_ref, other_ref, y_other, w_other)
    copy.wait()

    def hot_shells(source, c):
        hot = []
        for side in range(2):
            half = parity if side == 0 else 1 - parity
            shell = own_ref[pl.ds(source * stride + c * 2 + half, 1), :]
            hot.append((iota((SHELLS, LANES), 0).astype(F32) == shell).astype(F32))
        return jnp.concatenate(hot, axis=1).astype(BF16)

    def harmonic_rows(source, c, y_ref):
        start = ((source // 8) * per_peer + c) * BLOCK + source % 8
        return y_ref[pl.ds(start, PAD, stride=9), :]

    def forward(turn, carry):
        for place in range(step * per_peer):
            source, c = turn * step + place // per_peer, place % per_peer
            row = source * per_peer + c
            weighted = [
                harmonic_rows(source, c, y_ref) * w_ref[pl.ds(row, 1), :]
                for y_ref, w_ref in ((y_own, w_own), (y_other, w_other))
            ]
            both = split_rows(jnp.concatenate(weighted, axis=1))
            made = lax.dot_general(
                both, hot_shells(source, c), (((1,), (1,)), ((), ())), preferred_element_type=F32
            )
            local = meta_smem[source, FIELDS * c + 3]
            sum_ref[pl.ds(local, PAD, stride=pitch), 0:SHELLS] += join_rows(made)
        return carry

    lax.fori_loop(0, devices // step, forward, 0)

    left = iota((owned, LANES), 1) < SHELLS
    row_rank = iota((SHELLS, LANES), 0).astype(F32)
    lane_rank = iota((SHELLS, LANES), 1).astype(F32)
    lane_rank = jnp.where(lane_rank < SHELLS, lane_rank, lane_rank - SHELLS)
    ratio = jnp.exp(jnp.abs(row_rank - lane_rank) * (-2.3 / SHELLS))
    kernel = jnp.exp(jnp.maximum(row_rank, lane_rank) * (-2.3 / SHELLS)) * 2.0
    before = None
    for degree in range(LMAX + 1):
        lines = []
        for k in range(degree * degree, (degree + 1) ** 2):
            line = sum_ref[k * pitch : k * pitch + owned, :]
            line = line + pltpu.roll(line, SHELLS, 1)
            lines.append(line)
            if k == HARM - 1:
                moment_ref[:, k * SHELLS : (k + 1) * SHELLS] = line[:, 0:SHELLS]
            elif k % 2 == 0:
                before = line
            else:
                moment_ref[:, (k - 1) * SHELLS : (k + 1) * SHELLS] = jnp.where(left, before, line)
        green = kernel * (4.0 * math.pi / (2 * degree + 1))
        kernel = kernel * ratio
        green = jnp.concatenate(two_parts(green), axis=1).astype(BF16)
        first, second = two_parts(jnp.concatenate(lines, axis=0))
        both = jnp.where(iota(first.shape, 1) < SHELLS, first, second).astype(BF16)
        made = jnp.dot(both, jnp.concatenate([green, green], axis=0), preferred_element_type=F32)
        made = made[:, 0:LANES] + made[:, LANES : 2 * LANES]
        for place, k in enumerate(range(degree * degree, (degree + 1) ** 2)):
            table_ref[k * pitch : k * pitch + owned, :] = made[place * owned : (place + 1) * owned, :]
    result = pltpu.make_async_copy(moment_ref, moment_hbm, out_sem)
    result.start()

    def split(turn, carry):
        for place in range(8):
            atom = turn * 8 + place
            first, second = two_parts(table_ref[pl.ds(atom, PAD, stride=pitch), :])
            both = jnp.where(iota((PAD, LANES), 1) < SHELLS, first, second)
            both = jnp.concatenate([both, jnp.zeros((SHELLS - PAD, LANES), F32)], axis=0)
            split_ref[pl.ds(pl.multiple_of(atom * SHELLS, SHELLS), SHELLS), :] = both.astype(BF16)
        return carry

    lax.fori_loop(0, owned // 8, split, 0)

    def evaluate(turn, carry):
        for place in range(step * per_peer):
            source, c = turn * step + place // per_peer, place % per_peer
            local = meta_smem[source, FIELDS * c + 3]
            table = split_ref[pl.ds(pl.multiple_of(local * SHELLS, SHELLS), SHELLS), :]
            hot = hot_shells(source, c)
            picked = jnp.dot(table, jnp.concatenate([hot, hot], axis=0), preferred_element_type=F32)
            at = ((source // 8) * per_peer + c) * 72 + source % 8
            for side, (y_ref, part_ref) in enumerate(((y_own, part_own), (y_other, part_other))):
                product = picked[0:PAD, side * LANES : (side + 1) * LANES] * harmonic_rows(source, c, y_ref)
                main = jnp.sum(product[0 : PAD - 8].reshape(PAD // 8 - 1, 8, LANES), axis=0)
                last = jnp.where(iota((8, LANES), 0) < HARM - (PAD - 8), product[PAD - 8 :], 0.0)
                part_ref[pl.ds(at, 8, stride=9), :] = main + last
        return carry

    lax.fori_loop(0, devices // step, evaluate, 0)

    def answer(group, carry):
        line = own_ref[pl.ds(group * 8 * stride + stride - 1, 8, stride=stride), :]
        for side, part_ref in enumerate((part_own, part_other)):
            half = parity if side == 0 else 1 - parity
            totals = [jnp.zeros((8, LANES), F32) for _ in range(batches)]
            for c in range(per_peer):
                start = pl.multiple_of((group * per_peer + c) * 72, 8)
                total = part_ref[pl.ds(start, 8), :]
                for i in range(1, 8):
                    total = total + part_ref[pl.ds(start + 9 * i, 8), :]
                total = jnp.where(column(line, c, 5) > 0.5, total, 0.0)
                batch = column(line, c, 4)
                totals = [old + jnp.where(batch == b, total, 0.0) for b, old in enumerate(totals)]
            for b in range(batches):
                at = group * 8 * (2 * batches) + half * batches + b
                reply_ref[pl.ds(at, 8, stride=2 * batches), :] = totals[b]
        return carry

    lax.fori_loop(0, groups, answer, 0)
    result.wait()


def body(
    point_coords,
    charge,
    shell_index,
    neighbours,
    neighbour_count,
    batch_load,
    atom_coords,
    owner_slot,
):
    batches, slots = neighbours.shape
    points = charge.shape[1]
    atoms = owner_slot.shape[0]
    count_gy = lax.axis_size("gy")
    devices = lax.axis_size("gx") * count_gy
    owned = atoms // devices
    rows = batches * slots
    per_peer = rows // devices
    stride = per_peer * (points // LANES) + batches * 4 + 1

    outgoing = pl.pallas_call(
        functools.partial(pack_kernel, devices),
        out_shape=jax.ShapeDtypeStruct((devices * stride, LANES), F32),
        in_specs=[SMEM] + [HBM] * 7,
        out_specs=VMEM,
        scratch_shapes=[
            pltpu.SMEM((batches,), jnp.int32),
            pltpu.VMEM((batches, slots), jnp.int32),
            pltpu.VMEM((atoms // LANES, LANES), jnp.int32),
            pltpu.VMEM((8, atoms), F32),
            pltpu.VMEM((batches, slots, points), jnp.int32),
            pltpu.VMEM((3, batches, points), F32),
            pltpu.VMEM((batches, points), F32),
            pltpu.SemaphoreType.DMA((7,)),
        ],
        compiler_params=pltpu.CompilerParams(vmem_limit_bytes=16 << 20),
        name="pack",
    )(
        batch_load,
        *(
            pltpu.with_memory_space_constraint(value, pltpu.HBM)
            for value in (
                neighbour_count,
                neighbours,
                owner_slot.reshape(atoms // LANES, LANES),
                atom_coords,
                shell_index,
                jnp.transpose(point_coords, (1, 0, 2)),
                charge,
            )
        ),
    )
    arrived = lax.all_to_all(
        outgoing.reshape(devices, stride, 1, LANES), ("gx", "gy"), split_axis=0, concat_axis=0, tiled=True
    ).reshape(devices * stride, LANES)
    swapped = lax.ppermute(arrived, "gy", [(i, i ^ 1) for i in range(count_gy)])
    parity = (lax.axis_index("gy") % 2).astype(jnp.int32).reshape(1)
    held = rows // 8 * BLOCK + SPILL
    y_own, w_own = pl.pallas_call(
        functools.partial(own_kernel, devices, per_peer, batches),
        out_shape=(jax.ShapeDtypeStruct((held, LANES), F32), jax.ShapeDtypeStruct((rows, LANES), F32)),
        in_specs=[VMEM],
        out_specs=(VMEM, VMEM),
        compiler_params=pltpu.CompilerParams(vmem_limit_bytes=24 << 20),
        cost_estimate=pl.CostEstimate(flops=2_000_000_000, bytes_accessed=1000, transcendentals=0),
        name="own",
    )(arrived)
    moments, reply = pl.pallas_call(
        functools.partial(owner_kernel, devices, per_peer, batches),
        out_shape=(
            jax.ShapeDtypeStruct((owned, HARM * SHELLS), F32),
            jax.ShapeDtypeStruct((devices * 2 * batches, LANES), F32),
        ),
        in_specs=[SMEM] + [VMEM] * 4,
        out_specs=(HBM, VMEM),
        scratch_shapes=[
            pltpu.VMEM((held, LANES), F32),
            pltpu.VMEM((rows, LANES), F32),
            pltpu.VMEM((PAD * (owned + 1), LANES), F32),
            pltpu.VMEM((PAD * (owned + 1), LANES), F32),
            pltpu.VMEM((owned * SHELLS, LANES), BF16),
            pltpu.VMEM((rows * 9, LANES), F32),
            pltpu.VMEM((rows * 9, LANES), F32),
            pltpu.VMEM((owned, HARM * SHELLS), F32),
            pltpu.VMEM((devices, LANES), jnp.int32),
            pltpu.SMEM((devices, LANES), jnp.int32),
            pltpu.SemaphoreType.DMA,
            pltpu.SemaphoreType.DMA,
        ],
        compiler_params=pltpu.CompilerParams(vmem_limit_bytes=24 << 20),
        name="owner",
    )(parity, arrived, swapped, y_own, w_own)
    returned = lax.all_to_all(
        reply.reshape(devices, 2 * batches, LANES), ("gx", "gy"), split_axis=0, concat_axis=0, tiled=True
    )
    potential = jnp.sum(returned, axis=0).reshape(2, batches, LANES)
    return jnp.transpose(potential, (1, 0, 2)).reshape(batches, points), moments


def solution(mesh):
    return jax.shard_map(
        body,
        mesh=mesh,
        in_specs=(
            P(("gx", "gy"), None, None),
            P(("gx", "gy"), None),
            P(("gx", "gy"), None, None),
            P(("gx", "gy"), None),
            P(("gx", "gy")),
            P(("gx", "gy")),
            P(),
            P(),
        ),
        out_specs=(P(("gx", "gy"), None), P(("gx", "gy"), None)),
        check_vma=False,
    )
```

```python
import functools
import math

import jax
import jax.numpy as jnp
from jax import lax
from jax.experimental import pallas as pl
from jax.experimental.pallas import tpu as pltpu
from jax.sharding import PartitionSpec as P

SHELLS = 64
LMAX = 6
HARM = (LMAX + 1) ** 2
PAD = 56
SOFTEN = 0.01
LANES = 128
FIELDS = 8
BLOCK = 448
SPILL = 64
ROWS_AT_ONCE = 128
VMEM = pl.BlockSpec(memory_space=pltpu.VMEM)
SMEM = pl.BlockSpec(memory_space=pltpu.SMEM)
HBM = pl.BlockSpec(memory_space=pltpu.HBM)
F32 = jnp.float32
BF16 = jnp.bfloat16


def iota(shape, axis):
    return lax.broadcasted_iota(jnp.int32, shape, axis)


def three_parts(value):
    first = value.astype(BF16)
    rest = value - first.astype(F32)
    second = rest.astype(BF16)
    third = (rest - second.astype(F32)).astype(BF16)
    return first, second, third


def pack_kernel(
    devices,
    load_ref,
    count_hbm,
    label_hbm,
    slot_hbm,
    atom_hbm,
    shell_hbm,
    coord_hbm,
    charge_hbm,
    out_ref,
    count_ref,
    label_ref,
    slot_ref,
    table_ref,
    shell_ref,
    coord_ref,
    charge_ref,
    sems,
):
    copies = [
        pltpu.make_async_copy(source, into, sems.at[place])
        for place, (source, into) in enumerate(
            (
                (label_hbm, label_ref),
                (slot_hbm, slot_ref),
                (atom_hbm, table_ref.at[0:3, :]),
                (shell_hbm, shell_ref),
                (coord_hbm, coord_ref),
                (charge_hbm, charge_ref),
                (count_hbm, count_ref),
            )
        )
    ]
    for copy in copies:
        copy.start()
    batches, slots = label_ref.shape
    rows = batches * slots
    atoms = table_ref.shape[1]
    owned = atoms // devices
    per_peer = rows // devices
    halves = charge_ref.shape[1] // LANES
    stride = out_ref.shape[0] // devices

    for copy in copies[0:3]:
        copy.wait()
    for tile in range(atoms // LANES):
        table_ref[3:4, tile * LANES : (tile + 1) * LANES] = slot_ref[tile : tile + 1, :].astype(F32)
    label = jnp.concatenate([label_ref[b : b + 1, :] for b in range(batches)], axis=1)
    label = jnp.broadcast_to(label, (8, rows))
    high = lax.shift_right_logical(label, 7)
    low = lax.bitwise_and(label, 127)
    kept = iota((8, rows), 0) < 4
    found = jnp.zeros((8, rows), F32)
    for tile in range(atoms // LANES):
        piece = table_ref[:, tile * LANES : (tile + 1) * LANES]
        picked = jnp.take_along_axis(piece, low, axis=1, mode="promise_in_bounds")
        found = jnp.where((high == tile) & kept, picked, found)
    slot = found[3:4, :]
    owner = jnp.floor((slot + 0.5) * (1.0 / owned))
    local = slot - owner * owned

    for copy in copies[3:]:
        copy.wait()
    lane = iota((1, rows), 1)
    batch_row = jnp.zeros((1, rows), F32)
    live_row = jnp.zeros((1, rows), F32)
    for b in range(batches):
        inside = (lane >= b * slots) & (lane < (b + 1) * slots)
        batch_row = jnp.where(inside, float(b), batch_row)
        alive = inside & (lane - b * slots < count_ref[b]) & (load_ref[0] > b)
        live_row = jnp.where(alive, 1.0, live_row)
    sub = iota((8, rows), 0)
    fields = found
    for place, value in ((3, local), (4, batch_row), (5, live_row), (6, owner)):
        fields = jnp.where(sub == place, jnp.broadcast_to(value, (8, rows)), fields)
    columns = jnp.concatenate([fields, jnp.zeros((LANES - 8, rows), F32)], axis=0).T

    owner_column = columns[:, 6:7]
    earlier = (owner_column == owner) & (iota((rows, rows), 0) < iota((rows, rows), 1))
    rank = jnp.sum(earlier.astype(F32), axis=0, keepdims=True)
    target = (rank * devices + owner).astype(jnp.int32)
    order = (iota((rows, rows), 0) == target).astype(F32).astype(BF16)

    shells = shell_ref[...].reshape(rows, halves * LANES).astype(F32).astype(BF16)
    moved = jnp.dot(order, shells, preferred_element_type=F32)
    meta = sum(jnp.dot(order, part, preferred_element_type=F32) for part in three_parts(columns))
    for group in range(devices // 8):
        base = group * 8 * stride
        total = jnp.zeros((8, LANES), F32)
        for c in range(per_peer):
            first = c * devices + group * 8
            for h in range(halves):
                out_ref[pl.ds(base + c * halves + h, 8, stride=stride), :] = moved[
                    first : first + 8, h * LANES : (h + 1) * LANES
                ]
            piece = meta[first : first + 8, :]
            total = total + (pltpu.roll(piece, FIELDS * c, 1) if c else piece)
        out_ref[pl.ds(base + stride - 1, 8, stride=stride), :] = total

    odd = lax.bitwise_and(iota((8, LANES), 0), 1) == 1
    slot_rank = iota((slots, 1), 0)
    for b in range(batches):
        squared = jnp.zeros((slots, halves * LANES), F32)
        for axis in range(3):
            place = columns[b * slots : (b + 1) * slots, axis : axis + 1]
            offset = coord_ref[axis, b : b + 1, :] - place
            squared = squared + offset * offset
        close = jnp.where(slot_rank < count_ref[b], 1.0 / (1.0 + squared), 0.0)
        live = jnp.where(load_ref[0] > b, 1.0, 0.0)
        weight = charge_ref[b : b + 1, :] * live / jnp.sum(close, axis=0, keepdims=True)
        for quantity in range(4):
            line = coord_ref[quantity, b : b + 1, :] if quantity < 3 else weight
            value = jnp.where(odd, line[:, LANES : 2 * LANES], line[:, 0:LANES])
            for group in range(devices // 8):
                at = group * 8 * stride + per_peer * halves + b * 4 + quantity
                out_ref[pl.ds(at, 8, stride=stride), :] = value


def harmonics(x, y, z):
    def factor(degree, azimuth):
        norm = math.sqrt(
            (2 * degree + 1) / (4 * math.pi) * math.factorial(degree - azimuth) / math.factorial(degree + azimuth)
        )
        return norm * (math.sqrt(2.0) if azimuth else 1.0)

    cosine, sine = None, None
    for azimuth in range(LMAX + 1):
        if azimuth == 1:
            cosine, sine = x, y
        elif azimuth > 1:
            cosine, sine = cosine * x - sine * y, cosine * y + sine * x
        older, newer = None, None
        for degree in range(azimuth, LMAX + 1):
            if degree == azimuth:
                value = float(math.prod(range(1, 2 * azimuth, 2))) * factor(degree, azimuth)
            elif degree == azimuth + 1:
                value = z * ((2 * azimuth + 1) * newer / factor(degree - 1, azimuth) * factor(degree, azimuth))
            else:
                up = (2 * degree - 1) / (degree - azimuth) * factor(degree, azimuth) / factor(degree - 1, azimuth)
                down = (degree + azimuth - 1) / (degree - azimuth) * factor(degree, azimuth) / factor(degree - 2, azimuth)
                value = (z * up) * newer - down * older
            older, newer = newer, value
            middle = degree * degree + degree
            if azimuth == 0:
                yield middle, value
            else:
                yield middle + azimuth, cosine * value
                yield middle - azimuth, sine * value


def split_rows(value):
    main, tail = value[0 : PAD - 8], value[PAD - 8 : PAD]
    first = main.astype(BF16)
    second = (main - first.astype(F32)).astype(BF16)
    last = tail.astype(BF16).astype(F32)
    last = jnp.concatenate([last, tail - last], axis=0).astype(BF16)
    return jnp.concatenate([first, last, second], axis=0)


def join_rows(value):
    main = value[0 : PAD - 8] + value[PAD + 8 :]
    return jnp.concatenate([main, value[PAD - 8 : PAD] + value[PAD : PAD + 8]], axis=0)


def two_parts(value):
    first = value.astype(BF16).astype(F32)
    return first, value - first


def column(line, c, field):
    at = FIELDS * c + field
    return jnp.broadcast_to(line[:, at : at + 1], (8, LANES))


def geometry(devices, per_peer, batches, own_ref, source, y_ref, w_ref):
    stride = own_ref.shape[0] // devices
    shell_rows = per_peer * 2
    y_ref[pl.ds(devices * per_peer // 8 * BLOCK, SPILL), :] = jnp.zeros((SPILL, LANES), F32)

    def one(group, carry):
        base = group * 8 * stride
        line = own_ref[pl.ds(base + stride - 1, 8, stride=stride), :]
        points = [
            [source[pl.ds(base + shell_rows + b * 4 + i, 8, stride=stride), :] for i in range(4)]
            for b in range(batches)
        ]
        for c in range(per_peer):
            batch = column(line, c, 4)
            chosen = list(points[0])
            for b in range(1, batches):
                chosen = [jnp.where(batch == b, new, old) for new, old in zip(points[b], chosen)]
            offset = [chosen[i] - column(line, c, i) for i in range(3)]
            squared = offset[0] * offset[0] + offset[1] * offset[1] + offset[2] * offset[2]
            scale = lax.rsqrt(squared + SOFTEN)
            weight = jnp.where(column(line, c, 5) > 0.5, chosen[3] / (1.0 + squared), 0.0)
            w_ref[pl.ds(group * 8 * per_peer + c, 8, stride=per_peer), :] = weight
            start = pl.multiple_of((group * per_peer + c) * BLOCK, 8)
            for k, value in harmonics(*(part * scale for part in offset)):
                y_ref[pl.ds(start + k * 9, 8), :] = jnp.broadcast_to(value, (8, LANES))
        return carry

    lax.fori_loop(0, devices // 8, one, 0)


def own_kernel(devices, per_peer, batches, own_ref, y_ref, w_ref, meta_ref):
    stride = own_ref.shape[0] // devices
    for group in range(devices // 8):
        line = own_ref[pl.ds(group * 8 * stride + stride - 1, 8, stride=stride), :]
        meta_ref[group * 8 : group * 8 + 8, :] = line.astype(jnp.int32)
    geometry(devices, per_peer, batches, own_ref, own_ref, y_ref, w_ref)


def owner_kernel(
    devices,
    per_peer,
    batches,
    parity_ref,
    own_ref,
    other_ref,
    y_own,
    w_own,
    meta_ref,
    moment_hbm,
    reply_ref,
    y_other,
    w_other,
    sum_ref,
    table_ref,
    split_ref,
    part_own,
    part_other,
    moment_ref,
    meta_smem,
    sem,
    out_sem,
):
    stride = own_ref.shape[0] // devices
    groups = devices // 8
    owned = moment_ref.shape[0]
    pitch = owned + 1
    parity = parity_ref[0]
    step = max(1, ROWS_AT_ONCE // per_peer)

    copy = pltpu.make_async_copy(meta_ref, meta_smem, sem)
    copy.start()

    sum_ref[...] = jnp.zeros_like(sum_ref)
    table_ref[HARM * pitch :, :] = jnp.zeros(((PAD - HARM) * pitch, LANES), F32)

    geometry(devices, per_peer, batches, own_ref, other_ref, y_other, w_other)
    copy.wait()

    def hot_shells(source, c):
        hot = []
        for side in range(2):
            half = parity if side == 0 else 1 - parity
            shell = own_ref[pl.ds(source * stride + c * 2 + half, 1), :]
            hot.append((iota((SHELLS, LANES), 0).astype(F32) == shell).astype(F32))
        return jnp.concatenate(hot, axis=1).astype(BF16)

    def harmonic_rows(source, c, y_ref):
        start = ((source // 8) * per_peer + c) * BLOCK + source % 8
        return y_ref[pl.ds(start, PAD, stride=9), :]

    def forward(turn, carry):
        for place in range(step * per_peer):
            source, c = turn * step + place // per_peer, place % per_peer
            row = source * per_peer + c
            weighted = [
                harmonic_rows(source, c, y_ref) * w_ref[pl.ds(row, 1), :]
                for y_ref, w_ref in ((y_own, w_own), (y_other, w_other))
            ]
            both = split_rows(jnp.concatenate(weighted, axis=1))
            made = lax.dot_general(
                both, hot_shells(source, c), (((1,), (1,)), ((), ())), preferred_element_type=F32
            )
            local = meta_smem[source, FIELDS * c + 3]
            sum_ref[pl.ds(local, PAD, stride=pitch), 0:SHELLS] += join_rows(made)
        return carry

    lax.fori_loop(0, devices // step, forward, 0)

    left = iota((owned, LANES), 1) < SHELLS
    row_rank = iota((SHELLS, LANES), 0).astype(F32)
    lane_rank = iota((SHELLS, LANES), 1).astype(F32)
    lane_rank = jnp.where(lane_rank < SHELLS, lane_rank, lane_rank - SHELLS)
    ratio = jnp.exp(jnp.abs(row_rank - lane_rank) * (-2.3 / SHELLS))
    kernel = jnp.exp(jnp.maximum(row_rank, lane_rank) * (-2.3 / SHELLS)) * 2.0
    before = None
    for degree in range(LMAX + 1):
        lines = []
        for k in range(degree * degree, (degree + 1) ** 2):
            line = sum_ref[k * pitch : k * pitch + owned, :]
            line = line + pltpu.roll(line, SHELLS, 1)
            lines.append(line)
            if k == HARM - 1:
                moment_ref[:, k * SHELLS : (k + 1) * SHELLS] = line[:, 0:SHELLS]
            elif k % 2 == 0:
                before = line
            else:
                moment_ref[:, (k - 1) * SHELLS : (k + 1) * SHELLS] = jnp.where(left, before, line)
        green = kernel * (4.0 * math.pi / (2 * degree + 1))
        kernel = kernel * ratio
        green = jnp.concatenate(two_parts(green), axis=1).astype(BF16)
        first, second = two_parts(jnp.concatenate(lines, axis=0))
        both = jnp.where(iota(first.shape, 1) < SHELLS, first, second).astype(BF16)
        made = jnp.dot(both, jnp.concatenate([green, green], axis=0), preferred_element_type=F32)
        made = made[:, 0:LANES] + made[:, LANES : 2 * LANES]
        for place, k in enumerate(range(degree * degree, (degree + 1) ** 2)):
            table_ref[k * pitch : k * pitch + owned, :] = made[place * owned : (place + 1) * owned, :]
    result = pltpu.make_async_copy(moment_ref, moment_hbm, out_sem)
    result.start()

    def split(turn, carry):
        for place in range(8):
            atom = turn * 8 + place
            first, second = two_parts(table_ref[pl.ds(atom, PAD, stride=pitch), :])
            both = jnp.where(iota((PAD, LANES), 1) < SHELLS, first, second)
            both = jnp.concatenate([both, jnp.zeros((SHELLS - PAD, LANES), F32)], axis=0)
            split_ref[pl.ds(pl.multiple_of(atom * SHELLS, SHELLS), SHELLS), :] = both.astype(BF16)
        return carry

    lax.fori_loop(0, owned // 8, split, 0)

    def evaluate(turn, carry):
        for place in range(step * per_peer):
            source, c = turn * step + place // per_peer, place % per_peer
            local = meta_smem[source, FIELDS * c + 3]
            table = split_ref[pl.ds(pl.multiple_of(local * SHELLS, SHELLS), SHELLS), :]
            hot = hot_shells(source, c)
            picked = jnp.dot(table, jnp.concatenate([hot, hot], axis=0), preferred_element_type=F32)
            at = ((source // 8) * per_peer + c) * 72 + source % 8
            for side, (y_ref, part_ref) in enumerate(((y_own, part_own), (y_other, part_other))):
                product = picked[0:PAD, side * LANES : (side + 1) * LANES] * harmonic_rows(source, c, y_ref)
                main = jnp.sum(product[0 : PAD - 8].reshape(PAD // 8 - 1, 8, LANES), axis=0)
                last = jnp.where(iota((8, LANES), 0) < HARM - (PAD - 8), product[PAD - 8 :], 0.0)
                part_ref[pl.ds(at, 8, stride=9), :] = main + last
        return carry

    lax.fori_loop(0, devices // step, evaluate, 0)

    def answer(group, carry):
        line = own_ref[pl.ds(group * 8 * stride + stride - 1, 8, stride=stride), :]
        for side, part_ref in enumerate((part_own, part_other)):
            half = parity if side == 0 else 1 - parity
            totals = [jnp.zeros((8, LANES), F32) for _ in range(batches)]
            for c in range(per_peer):
                start = pl.multiple_of((group * per_peer + c) * 72, 8)
                total = part_ref[pl.ds(start, 8), :]
                for i in range(1, 8):
                    total = total + part_ref[pl.ds(start + 9 * i, 8), :]
                total = jnp.where(column(line, c, 5) > 0.5, total, 0.0)
                batch = column(line, c, 4)
                totals = [old + jnp.where(batch == b, total, 0.0) for b, old in enumerate(totals)]
            for b in range(batches):
                at = group * 8 * (2 * batches) + half * batches + b
                reply_ref[pl.ds(at, 8, stride=2 * batches), :] = totals[b]
        return carry

    lax.fori_loop(0, groups, answer, 0)
    result.wait()


def body(
    point_coords,
    charge,
    shell_index,
    neighbours,
    neighbour_count,
    batch_load,
    atom_coords,
    owner_slot,
):
    batches, slots = neighbours.shape
    points = charge.shape[1]
    atoms = owner_slot.shape[0]
    count_gy = lax.axis_size("gy")
    devices = lax.axis_size("gx") * count_gy
    owned = atoms // devices
    rows = batches * slots
    per_peer = rows // devices
    stride = per_peer * (points // LANES) + batches * 4 + 1

    outgoing = pl.pallas_call(
        functools.partial(pack_kernel, devices),
        out_shape=jax.ShapeDtypeStruct((devices * stride, LANES), F32),
        in_specs=[SMEM] + [HBM] * 7,
        out_specs=VMEM,
        scratch_shapes=[
            pltpu.SMEM((batches,), jnp.int32),
            pltpu.VMEM((batches, slots), jnp.int32),
            pltpu.VMEM((atoms // LANES, LANES), jnp.int32),
            pltpu.VMEM((8, atoms), F32),
            pltpu.VMEM((batches, slots, points), jnp.int32),
            pltpu.VMEM((3, batches, points), F32),
            pltpu.VMEM((batches, points), F32),
            pltpu.SemaphoreType.DMA((7,)),
        ],
        compiler_params=pltpu.CompilerParams(vmem_limit_bytes=16 << 20),
        name="pack",
    )(
        batch_load,
        *(
            pltpu.with_memory_space_constraint(value, pltpu.HBM)
            for value in (
                neighbour_count,
                neighbours,
                owner_slot.reshape(atoms // LANES, LANES),
                atom_coords,
                shell_index,
                jnp.transpose(point_coords, (1, 0, 2)),
                charge,
            )
        ),
    )
    arrived = lax.all_to_all(
        outgoing.reshape(devices, stride, 1, LANES), ("gx", "gy"), split_axis=0, concat_axis=0, tiled=True
    ).reshape(devices * stride, LANES)
    swapped = lax.ppermute(arrived, "gy", [(i, i ^ 1) for i in range(count_gy)])
    parity = (lax.axis_index("gy") % 2).astype(jnp.int32).reshape(1)
    held = rows // 8 * BLOCK + SPILL
    y_own, w_own, meta = pl.pallas_call(
        functools.partial(own_kernel, devices, per_peer, batches),
        out_shape=(
            jax.ShapeDtypeStruct((held, LANES), F32),
            jax.ShapeDtypeStruct((rows, LANES), F32),
            jax.ShapeDtypeStruct((devices, LANES), jnp.int32),
        ),
        in_specs=[VMEM],
        out_specs=(VMEM, VMEM, VMEM),
        compiler_params=pltpu.CompilerParams(vmem_limit_bytes=24 << 20),
        cost_estimate=pl.CostEstimate(flops=2_000_000_000, bytes_accessed=1000, transcendentals=0),
        name="own",
    )(arrived)
    moments, reply = pl.pallas_call(
        functools.partial(owner_kernel, devices, per_peer, batches),
        out_shape=(
            jax.ShapeDtypeStruct((owned, HARM * SHELLS), F32),
            jax.ShapeDtypeStruct((devices * 2 * batches, LANES), F32),
        ),
        in_specs=[SMEM] + [VMEM] * 5,
        out_specs=(HBM, VMEM),
        scratch_shapes=[
            pltpu.VMEM((held, LANES), F32),
            pltpu.VMEM((rows, LANES), F32),
            pltpu.VMEM((PAD * (owned + 1), LANES), F32),
            pltpu.VMEM((PAD * (owned + 1), LANES), F32),
            pltpu.VMEM((owned * SHELLS, LANES), BF16),
            pltpu.VMEM((rows * 9, LANES), F32),
            pltpu.VMEM((rows * 9, LANES), F32),
            pltpu.VMEM((owned, HARM * SHELLS), F32),
            pltpu.SMEM((devices, LANES), jnp.int32),
            pltpu.SemaphoreType.DMA,
            pltpu.SemaphoreType.DMA,
        ],
        compiler_params=pltpu.CompilerParams(vmem_limit_bytes=24 << 20),
        name="owner",
    )(parity, arrived, swapped, y_own, w_own, meta)
    returned = lax.all_to_all(
        reply.reshape(devices, 2 * batches, 1, LANES), ("gx", "gy"), split_axis=0, concat_axis=0, tiled=True
    ).reshape(devices, 2 * batches, LANES)
    potential = jnp.sum(returned, axis=0).reshape(2, batches, LANES)
    return jnp.transpose(potential, (1, 0, 2)).reshape(batches, points), moments


def solution(mesh):
    return jax.shard_map(
        body,
        mesh=mesh,
        in_specs=(
            P(("gx", "gy"), None, None),
            P(("gx", "gy"), None),
            P(("gx", "gy"), None, None),
            P(("gx", "gy"), None),
            P(("gx", "gy")),
            P(("gx", "gy")),
            P(),
            P(),
        ),
        out_specs=(P(("gx", "gy"), None), P(("gx", "gy"), None)),
        check_vma=False,
    )
```
